512 devices in a mesh: rep: 2 (over y), exp: 16 (over x, core), tp: 16 (over z).
Axes of the slice: x: 8, y: 2, z: 16, core: 2. Of those that a mesh axis runs over, the one named last changes fastest.
The devices are a block of a 8x8x16 slice.
Arguments:
- tokens: bfloat16 [1024, 6144], P(('rep', 'exp'), 'tp'), parts along dimension 0, may hold values from -6 to 6
- expert_ids: int32 [1024, 2], P(('rep', 'exp')), parts along dimension 0, may hold values from 0 to 3, all different within a row; in each aligned block of 32 rows (0 to 31, 32 to 63, ...) at most 20 rows name the same one
- route_logits: float32 [1024, 2], P(('rep', 'exp')), parts along dimension 0, may hold values from -6 to 6
- gate_weight: bfloat16 [6144, 32768], P(None, ('exp', 'tp')), may hold values from -0.078125 to 0.078125
- up_weight: bfloat16 [6144, 32768], P(None, ('exp', 'tp')), may hold values from -0.078125 to 0.078125
- down_weight: bfloat16 [32768, 6144], P(('exp', 'tp')), may hold values from -0.0625 to 0.0625
Outputs:
- moe_out: bfloat16 [1024, 6144], P(('rep', 'exp'), 'tp'), parts along dimension 0
The draws below stay inside these ranges and needn't reach their ends.
There are 2 independent parts, one for each index of `rep`. The reference program is written for one: setup_inputs(seed, part) draws one part's arguments, and reference() takes and returns one part's arrays. A program takes and returns all parts, laid end to end along the dimension named above; an argument that names none is the same for every part. Nothing has to cross between parts.
Inputs may be any that keep to these rules, and one draw needn't show every extreme that they name: `expert_ids`: each token names two different experts. In each aligned block of 32 tokens no expert is named by more than 20 tokens, a bound that some block reaches.
All inputs are finite; a program needn't handle non-finite values.
Results may differ from the reference program's by a relative error of at most 0.019.
Values may be sent and summed in bfloat16 or wider, within the bound.
No kernel may reach another device: no remote copies, remote signals or barrier semaphores. Data moves between devices by JAX's collectives and lax.ppermute only.
A program may use at most 64 MiB of HBM per device.

```python
import math
import jax
import jax.numpy as jnp
import numpy as np
from jax import lax

D = 6144
FF = 8192
EXPERTS = 4
TOK_EXP = 32
CAP = 20
TOKENS = 512
N_EXP = 16
N_TP = 16


def steps_of(rng, extent, cuts, low, largest):
    gain, own = 1.0, jax.random.fold_in(rng, 6)
    for dim, parts in cuts:
        draws = jnp.exp(jax.random.uniform(jax.random.fold_in(own, dim), (parts,), jnp.float32, low / len(cuts), largest / len(cuts)))
        gain = gain * jnp.repeat(draws, extent[dim] // parts).reshape([-1 if axis == dim else 1 for axis in range(len(extent))])
    return gain


def routed_block(rng, own, number, rows, count, top, bound, lean):
    order = jax.random.permutation(rng, count)
    packed, common = portions_of(count, rows * top, bound, lean, True), portions_of(count, rows * top, bound, lean, False)
    places = jnp.arange(count)

    def named(lengths, rotation):
        used = int((lengths > 0).sum())
        fixed = max(1, used // 4)
        passed = fixed + (places - fixed + rotation * (used - fixed)) % max(1, count - fixed)
        return jnp.zeros((count,), jnp.int32).at[order[jnp.where(places < fixed, places, passed)]].set(jnp.asarray(lengths, jnp.int32))

    lengths = jnp.where(number % 4 == 0, named(packed, number // 4), named(common, number - number // 4 - 1))
    mixed = jax.random.permutation(jax.random.fold_in(own, 3), count)
    source_of, taker = mixed[0:count // 2 * 2:2], mixed[1:count // 2 * 2:2]
    room = jnp.minimum(lengths[source_of] - 1, bound - lengths[taker]) // 2
    room = jnp.where((source_of == order[0]) | (taker == order[0]) | (lengths[taker] == 0), 0, jnp.maximum(room, 0))
    passed = jax.random.randint(jax.random.fold_in(own, 4), (count // 2,), 0, 1 << 20) % (room + 1)
    lengths = lengths.at[source_of].add(-passed).at[taker].add(passed)
    members = jnp.searchsorted(jnp.cumsum(lengths), jnp.arange(rows * top), side="right").astype(jnp.int32)
    listing = members.reshape(top, rows).T
    listing = listing[jax.random.permutation(jax.random.fold_in(own, 1), rows)]
    rotation = jax.random.randint(jax.random.fold_in(own, 2), (rows, 1), 0, top)
    return jnp.take_along_axis(listing, (jnp.arange(top)[None, :] + rotation) % top, axis=1)


def portions_of(number_of, total, reach, skew, full):
    portions = [(1 << 20) // math.isqrt(rank ** skew) + 1 for rank in range(1, number_of + 1)]
    largest = reach if full else min(reach, max(-(-total // number_of), total * portions[0] // sum(portions)))
    least = 1 if total - largest >= number_of - 1 else 0
    counts, spare = [largest] + [least] * (number_of - 1), total - largest - least * (number_of - 1)
    while spare > 0:
        candidates = [i for i in range(1, number_of) if counts[i] < largest] or [i for i in range(1, number_of) if counts[i] < reach]
        pool, remaining = sum([portions[i] for i in candidates]), spare
        for i in candidates:
            more = min(reach - counts[i], max(1, remaining * portions[i] // pool), spare)
            counts[i] = counts[i] + more
            spare = spare - more
    return np.array(counts)


def normal_values(rng, dims, scale, reach, split=(), kind=jnp.bfloat16):
    array = scale * jax.random.normal(rng, dims, jnp.float32)
    if split:
        array = array * steps_of(rng, dims, split, -0.22, 0.18)
    return jnp.clip(array, -reach, reach).astype(kind)


def setup_inputs(seed: int = 0, part: int = 0) -> dict:
    splits = jax.random.split(jax.random.key(seed), 7)
    own_keys = jax.random.split(jax.random.fold_in(splits[6], part), 7)
    tokens = normal_values(own_keys[0], (TOKENS, D), 1.0, 6.0, ((0, 16), (1, 16)))
    expert_ids_keys = jax.random.split(jax.random.fold_in(own_keys[1], 1), TOKENS // TOK_EXP)
    expert_ids_turns = jax.random.permutation(jax.random.fold_in(own_keys[1], 3), TOKENS // TOK_EXP)
    expert_ids = jax.vmap(lambda own, number: routed_block(jax.random.fold_in(own_keys[1], 2), own, number, TOK_EXP, EXPERTS, 2, CAP, 2))(expert_ids_keys, expert_ids_turns).reshape((TOKENS, 2))
    route_logits = normal_values(own_keys[2], (TOKENS, 2), 1.5, 6.0, ((0, 16),), jnp.float32)
    gate_weight = normal_values(splits[3], (D, EXPERTS * FF), D ** -0.5, 0.078125, ((1, 256),))
    up_weight = normal_values(splits[4], (D, EXPERTS * FF), D ** -0.5, 0.078125, ((1, 256),))
    down_weight = normal_values(splits[5], (EXPERTS * FF, D), FF ** -0.5, 0.0625, ((0, 256),))
    return {"tokens": tokens, "expert_ids": expert_ids, "route_logits": route_logits, "gate_weight": gate_weight, "up_weight": up_weight, "down_weight": down_weight}


def slot_tables(expert_ids, route_logits):
    chosen = (expert_ids[:, :, None] == jnp.arange(EXPERTS, dtype=jnp.int32)[None, None, :]).astype(jnp.int32)
    per_token = jnp.sum(chosen, axis=1)
    before = jnp.cumsum(per_token, axis=0) - per_token
    position = jnp.sum(chosen * before[:, None, :], axis=2)
    at_slot = (position[:, :, None] == jnp.arange(CAP, dtype=jnp.int32)[None, None, :]).astype(jnp.float32)
    chosen_f = chosen.astype(jnp.float32)
    diff = route_logits[:, 0] - route_logits[:, 1]
    shares = jnp.stack([jax.nn.sigmoid(diff), jax.nn.sigmoid(-diff)], axis=1)
    placement = jnp.einsum('tke,tkc->ect', chosen_f, at_slot)
    mixing = jnp.einsum('tk,tke,tkc->tec', shares, chosen_f, at_slot)
    return placement, mixing


def reference(tokens, expert_ids, route_logits, gate_weight, up_weight, down_weight):
    homes = tokens.reshape(N_EXP, TOK_EXP, D)
    placement, mixing = jax.vmap(slot_tables)(expert_ids.reshape(N_EXP, TOK_EXP, 2), route_logits.reshape(N_EXP, TOK_EXP, 2))
    slots = jnp.einsum('hect,htd->ehcd', placement.astype(jnp.float32), homes.astype(jnp.float32)).astype(jnp.bfloat16)
    block_width = FF // (N_EXP // EXPERTS * N_TP)
    blocks = FF // block_width
    outputs = []
    for expert in range(EXPERTS):
        slot_rows = slots[expert].reshape(N_EXP * CAP, D)
        gate_act = jnp.dot(slot_rows, gate_weight[:, expert * FF:(expert + 1) * FF], preferred_element_type=jnp.float32)
        up_act = jnp.dot(slot_rows, up_weight[:, expert * FF:(expert + 1) * FF], preferred_element_type=jnp.float32)
        hidden = (jax.nn.silu(gate_act) * up_act).astype(jnp.bfloat16)
        hidden_blocks = jnp.transpose(hidden.reshape(N_EXP * CAP, blocks, block_width), (1, 0, 2))
        down_blocks = down_weight[expert * FF:(expert + 1) * FF].reshape(blocks, block_width, D)

        def add_block(running, piece_pair):
            term = jnp.dot(piece_pair[0], piece_pair[1], preferred_element_type=jnp.float32).astype(jnp.bfloat16)
            term = lax.optimization_barrier(term)
            return running + term.astype(jnp.float32), 0

        start = jnp.zeros((N_EXP * CAP, D), jnp.float32)
        summed, unused = lax.scan(add_block, start, (hidden_blocks, down_blocks))
        outputs.append(summed.reshape(N_EXP, CAP, D))
    expert_out = jnp.stack(outputs, axis=0)
    moe_out = jnp.einsum('htec,ehcd->htd', mixing, expert_out, precision=lax.Precision.HIGHEST)
    return moe_out.reshape(TOKENS, D).astype(jnp.bfloat16)
```

```python
import functools

import jax
import jax.numpy as jnp
from jax import lax
from jax.experimental import pallas as pl
from jax.experimental.pallas import tpu as pltpu
from jax.sharding import Mesh, PartitionSpec as P

EXPERTS = 4
CAP = 20
QUARTERS = 4
CORES = 2


def cost(flops, nbytes):
    return pl.CostEstimate(flops=flops, bytes_accessed=nbytes, transcendentals=0)


def count_at_least(index, width, parts):
    total = jnp.zeros_like(index)
    for k in range(1, parts):
        total = total + (index >= k * width).astype(jnp.int32)
    return total


def placed(ids, expert, slot, before):
    chosen = ((ids[0:1, :] == expert) | (ids[1:2, :] == expert)).astype(jnp.float32)
    position = jnp.dot(chosen, before, preferred_element_type=jnp.float32)
    return chosen * (position == slot.astype(jnp.float32)).astype(jnp.float32)


def dispatch_kernel(chips, ids_ref, tokens_ref, out_ref):
    count = tokens_ref.shape[0]
    rows = EXPERTS * CAP
    row = lax.broadcasted_iota(jnp.int32, (rows, count), 0)
    expert = count_at_least(row, CAP, EXPERTS)
    slot = row - CAP * expert
    first = lax.broadcasted_iota(jnp.int32, (count, count), 0)
    second = lax.broadcasted_iota(jnp.int32, (count, count), 1)
    before = (first < second).astype(jnp.float32)
    placement = placed(ids_ref[...], expert, slot, before).astype(jnp.bfloat16)
    slots = jnp.dot(placement, tokens_ref[...], preferred_element_type=jnp.float32).astype(
        jnp.bfloat16
    )
    per_expert = chips // EXPERTS
    for chip in range(chips):
        e = chip // per_expert
        out_ref[chip] = slots[e * CAP : (e + 1) * CAP]


def dispatch(ids, tokens, chips):
    features = tokens.shape[1]
    return pl.pallas_call(
        functools.partial(dispatch_kernel, chips),
        out_shape=jax.ShapeDtypeStruct((chips, CAP, features), jnp.bfloat16),
        cost_estimate=cost(2 * 80 * 32 * features, 200000),
        compiler_params=pltpu.CompilerParams(vmem_limit_bytes=4 << 20),
        name="dispatch",
    )(ids, tokens)


def mixing_kernel(chips, count, ids_ref, logits_ref, out_ref):
    lanes = ids_ref.shape[1]
    rows = chips * QUARTERS * CAP
    row = lax.broadcasted_iota(jnp.int32, (rows, lanes), 0)
    chip = count_at_least(row, QUARTERS * CAP, chips)
    rest = row - QUARTERS * CAP * chip
    quarter = count_at_least(rest, CAP, QUARTERS)
    slot = rest - CAP * quarter
    expert = count_at_least(chip, chips // EXPERTS, EXPERTS)
    lane = lax.broadcasted_iota(jnp.int32, (rows, lanes), 1)
    own = (count_at_least(lane, count, QUARTERS) == quarter).astype(jnp.float32)
    first = lax.broadcasted_iota(jnp.int32, (lanes, lanes), 0)
    second = lax.broadcasted_iota(jnp.int32, (lanes, lanes), 1)
    same = count_at_least(first, count, QUARTERS) == count_at_least(second, count, QUARTERS)
    before = ((first < second) & same).astype(jnp.float32)
    ids = ids_ref[...]
    diff = logits_ref[0:1, :] - logits_ref[1:2, :]
    share = jnp.where(ids[0:1, :] == expert, jax.nn.sigmoid(diff), jax.nn.sigmoid(-diff))
    out_ref[...] = (placed(ids, expert, slot, before) * share * own).astype(jnp.bfloat16)


def mixing(ids, logits, chips):
    count = ids.shape[1]
    rows = chips * QUARTERS * CAP
    return pl.pallas_call(
        functools.partial(mixing_kernel, chips, count),
        out_shape=jax.ShapeDtypeStruct((rows, QUARTERS * count), jnp.bfloat16),
        cost_estimate=cost(2 * rows * 128 * 128, 200000),
        compiler_params=pltpu.CompilerParams(vmem_limit_bytes=8 << 20),
        name="mixing",
    )(jnp.tile(ids, (1, QUARTERS)), jnp.tile(logits, (1, QUARTERS)))


def ffn_kernel(
    steps, chips, low_ref, high_ref, gate_ref, gate2_ref, up_ref, up2_ref, down_ref, down2_ref, out_ref, total, hidden
):
    step = pl.program_id(0)
    half = low_ref.shape[1]
    depth = low_ref.shape[2]
    blocks = low_ref.shape[0]

    @pl.when(step == 0)
    def _():
        total[...] = jnp.zeros_like(total)

    @pl.when(step < steps)
    def _():
        for part, ref in enumerate((low_ref, high_ref)):
            rows = slice(part * half, (part + 1) * half)
            added = total[rows]
            for b in range(blocks):
                k = slice(b * depth, (b + 1) * depth)
                weight = jnp.concatenate(
                    [gate_ref[k], gate2_ref[k], up_ref[k], up2_ref[k]], axis=1
                )
                added = added + jnp.dot(ref[b], weight, preferred_element_type=jnp.float32)
            total[rows] = added

    @pl.when(step == steps - 1)
    def _():
        width = total.shape[1] // 2
        gate = total[:, :width]
        hidden[...] = (gate * jax.nn.sigmoid(gate) * total[:, width:]).astype(jnp.bfloat16)

    for q in range(QUARTERS):

        @pl.when(step == steps + q)
        def _(q=q):
            weight = jnp.concatenate([down_ref[...], down2_ref[...]], axis=0)
            partial = jnp.dot(hidden[...], weight, preferred_element_type=jnp.float32)
            for chip in range(chips):
                out_ref[chip, q * CAP : (q + 1) * CAP, :] = partial[
                    chip * CAP : (chip + 1) * CAP
                ].astype(jnp.bfloat16)


def ffn(low, high, gate, gate2, up, up2, down, down2, chips):
    parts, half, depth = low.shape
    model, width = gate.shape
    steps = 4
    blocks = parts // steps
    quarter = model // QUARTERS
    rows = 2 * half
    into = lambda i: (jnp.minimum(i, steps - 1), 0, 0)
    weights = pl.BlockSpec((blocks * depth, width), lambda i: (jnp.minimum(i, steps - 1), 0))
    downs = pl.BlockSpec((width, quarter), lambda i: (0, jnp.maximum(i - steps, 0)))
    tokens_in = pl.BlockSpec((blocks, half, depth), into)
    return pl.pallas_call(
        functools.partial(ffn_kernel, steps, chips),
        grid=(steps + QUARTERS,),
        in_specs=[tokens_in, tokens_in, weights, weights, weights, weights, downs, downs],
        out_specs=pl.BlockSpec((chips, QUARTERS * CAP, quarter), lambda i: (0, 0, 0)),
        out_shape=jax.ShapeDtypeStruct((chips, QUARTERS * CAP, quarter), jnp.bfloat16),
        scratch_shapes=[
            pltpu.VMEM((rows, 4 * width), jnp.float32),
            pltpu.VMEM((rows, 2 * width), jnp.bfloat16),
        ],
        cost_estimate=cost(2 * rows * model * width * 6, 14000000),
        compiler_params=pltpu.CompilerParams(vmem_limit_bytes=24 << 20),
        name="ffn",
    )(low, high, gate, gate2, up, up2, down, down2)


def combine_kernel(mix_ref, back_ref, out_ref):
    blocks, count, depth = out_ref.shape
    per_quarter = blocks // QUARTERS
    summed = lax.dot_general(
        mix_ref[...], back_ref[...], (((0,), (0,)), ((), ())), preferred_element_type=jnp.float32
    ).astype(jnp.bfloat16)
    for q in range(QUARTERS):
        for s in range(per_quarter):
            out_ref[q * per_quarter + s] = summed[
                q * count : (q + 1) * count, s * depth : (s + 1) * depth
            ]


def combine(mix, back, count, blocks):
    rows, quarter = back.shape
    depth = QUARTERS * quarter // blocks
    return pl.pallas_call(
        combine_kernel,
        out_shape=jax.ShapeDtypeStruct((blocks, count, depth), jnp.bfloat16),
        cost_estimate=cost(2 * rows * quarter * 128, 2400000),
        compiler_params=pltpu.CompilerParams(vmem_limit_bytes=12 << 20),
        name="combine",
    )(mix, back)


def on_device(tokens, expert_ids, route_logits, gate_weight, up_weight, down_weight):
    chips = lax.axis_size("x")
    parts = lax.axis_size("tp")
    count, depth = tokens.shape
    swap = [(0, 1), (1, 0)]
    ids = expert_ids.T
    outgoing = dispatch(ids, tokens, chips)
    incoming = lax.all_to_all(outgoing, "x", 0, 0, tiled=True)
    gate2 = lax.ppermute(gate_weight, "core", swap)
    up2 = lax.ppermute(up_weight, "core", swap)
    down2 = lax.ppermute(down_weight, "core", swap)
    rows = incoming.reshape(2, chips * CAP // 2, depth)
    low = lax.all_gather(rows[0], "tp")
    high = lax.all_gather(rows[1], "tp")
    partial_value = ffn(low, high, gate_weight, gate2, up_weight, up2, down_weight, down2, chips)
    returned = lax.all_to_all(partial_value, "x", 0, 0, tiled=True)
    mix = mixing(ids, route_logits.T, chips)
    back = returned.reshape(chips * QUARTERS * CAP, parts * depth // QUARTERS)
    combined = combine(mix, back, count, parts)
    blocks = lax.all_to_all(combined, "tp", 0, 0, tiled=True)
    return jnp.sum(blocks.astype(jnp.float32), axis=0).astype(jnp.bfloat16)


def solution(mesh):
    sizes = [mesh.shape[axis] for axis in ("rep", "exp", "tp")]
    devices = mesh.devices.reshape(sizes[0], sizes[1] // CORES, CORES, sizes[2])
    split = Mesh(devices, ("rep", "x", "core", "tp"))
    tokens = ("rep", "x", "core")
    hidden = ("x", "core", "tp")
    return jax.shard_map(
        on_device,
        mesh=split,
        in_specs=(
            P(tokens, "tp"),
            P(tokens, None),
            P(tokens, None),
            P(None, hidden),
            P(None, hidden),
            P(hidden, None),
        ),
        out_specs=P(tokens, "tp"),
        check_vma=False,
    )
```

```python
import functools

import jax
import jax.numpy as jnp
from jax import lax
from jax.experimental import pallas as pl
from jax.experimental.pallas import tpu as pltpu
from jax.sharding import Mesh, PartitionSpec as P

EXPERTS = 4
CAP = 20
MAIN = 16
TAIL = CAP - MAIN
QUARTERS = 4
CORES = 2


def cost(flops, nbytes):
    return pl.CostEstimate(flops=flops, bytes_accessed=nbytes, transcendentals=0)


def count_at_least(index, width, parts):
    total = jnp.zeros_like(index)
    for k in range(1, parts):
        total = total + (index >= k * width).astype(jnp.int32)
    return total


def placed(ids, expert, slot, before):
    chosen = ((ids[0:1, :] == expert) | (ids[1:2, :] == expert)).astype(jnp.float32)
    position = jnp.dot(chosen, before, preferred_element_type=jnp.float32)
    return chosen * (position == slot.astype(jnp.float32)).astype(jnp.float32)


def grouped(row, groups):
    later = row >= groups * MAIN
    rest = row - groups * MAIN
    main = count_at_least(row, MAIN, groups)
    tail = count_at_least(rest, TAIL, groups)
    group = jnp.where(later, tail, main)
    slot = jnp.where(later, MAIN + rest - TAIL * tail, row - MAIN * main)
    return group, slot


def dispatch_kernel(chips, ids_ref, tokens_ref, out_ref, image, sems):
    blocks, count, depth = tokens_ref.shape
    per_quarter = blocks // QUARTERS
    per_expert = chips // EXPERTS
    row = lax.broadcasted_iota(jnp.int32, (EXPERTS * CAP, count), 0)
    expert, slot = grouped(row, EXPERTS)
    first = lax.broadcasted_iota(jnp.int32, (count, count), 0)
    second = lax.broadcasted_iota(jnp.int32, (count, count), 1)
    before = (first < second).astype(jnp.float32)
    placement = placed(ids_ref[...], expert, slot, before).astype(jnp.bfloat16)
    for b in range(blocks):
        q, s = b // per_quarter, b % per_quarter
        lanes = slice(s * depth, (s + 1) * depth)
        slots = jnp.dot(placement, tokens_ref[b], preferred_element_type=jnp.float32).astype(
            jnp.bfloat16
        )
        for e in range(EXPERTS):
            image[e, q * MAIN : (q + 1) * MAIN, lanes] = slots[e * MAIN : (e + 1) * MAIN]
            to, at = QUARTERS * MAIN + q * TAIL, EXPERTS * MAIN + e * TAIL
            image[e, to : to + TAIL, lanes] = slots[at : at + TAIL]
    copies = [
        pltpu.make_async_copy(image.at[chip // per_expert], out_ref.at[chip], sems.at[chip])
        for chip in range(chips)
    ]
    for copy in copies:
        copy.start()
    for copy in copies:
        copy.wait()


def dispatch(ids, tokens, chips):
    blocks, count, depth = tokens.shape
    quarter = blocks * depth // QUARTERS
    return pl.pallas_call(
        functools.partial(dispatch_kernel, chips),
        out_shape=jax.ShapeDtypeStruct((chips, QUARTERS * CAP, quarter), jnp.bfloat16),
        out_specs=pl.BlockSpec(memory_space=pltpu.HBM),
        scratch_shapes=[
            pltpu.VMEM((EXPERTS, QUARTERS * CAP, quarter), jnp.bfloat16),
            pltpu.SemaphoreType.DMA((chips,)),
        ],
        cost_estimate=cost(2 * 80 * count * blocks * depth, 2400000),
        compiler_params=pltpu.CompilerParams(vmem_limit_bytes=60 << 20),
        name="dispatch",
    )(ids, tokens)


def mixing_kernel(chips, count, ids_ref, logits_ref, out_ref):
    lanes = ids_ref.shape[1]
    rows = chips * QUARTERS * CAP
    row = lax.broadcasted_iota(jnp.int32, (rows, lanes), 0)
    chip = count_at_least(row, QUARTERS * CAP, chips)
    quarter, slot = grouped(row - QUARTERS * CAP * chip, QUARTERS)
    expert = count_at_least(chip, chips // EXPERTS, EXPERTS)
    lane = lax.broadcasted_iota(jnp.int32, (rows, lanes), 1)
    own = (count_at_least(lane, count, QUARTERS) == quarter).astype(jnp.float32)
    first = lax.broadcasted_iota(jnp.int32, (lanes, lanes), 0)
    second = lax.broadcasted_iota(jnp.int32, (lanes, lanes), 1)
    same = count_at_least(first, count, QUARTERS) == count_at_least(second, count, QUARTERS)
    before = ((first < second) & same).astype(jnp.float32)
    ids = ids_ref[...]
    diff = logits_ref[0:1, :] - logits_ref[1:2, :]
    share = jnp.where(ids[0:1, :] == expert, jax.nn.sigmoid(diff), jax.nn.sigmoid(-diff))
    out_ref[...] = (placed(ids, expert, slot, before) * share * own).astype(jnp.bfloat16)


def mixing(ids, logits, chips):
    count = ids.shape[1]
    rows = chips * QUARTERS * CAP
    return pl.pallas_call(
        functools.partial(mixing_kernel, chips, count),
        out_shape=jax.ShapeDtypeStruct((rows, QUARTERS * count), jnp.bfloat16),
        cost_estimate=cost(2 * rows * 128 * 128, 200000),
        compiler_params=pltpu.CompilerParams(vmem_limit_bytes=8 << 20),
        name="mixing",
    )(jnp.tile(ids, (1, QUARTERS)), jnp.tile(logits, (1, QUARTERS)))


def ffn_kernel(
    slots_ref, gate_ref, gate2_ref, up_ref, up2_ref, down_ref, down2_ref, out_ref, slots, ins, downs, outs, slot_sem, in_sems, out_sems
):
    chips, _, quarter = slots_ref.shape
    width = gate_ref.shape[1]
    mains = QUARTERS * MAIN
    arrival = pltpu.make_async_copy(slots_ref, slots, slot_sem)
    arrival.start()
    first, second = [], []
    for q in range(QUARTERS):
        k = pl.ds(q * quarter, quarter)
        first.append(
            [
                pltpu.make_async_copy(
                    ref.at[k], ins.at[q, :, pl.ds(i * width, width)], in_sems.at[q, i]
                )
                for i, ref in enumerate((gate_ref, gate2_ref, up_ref, up2_ref))
            ]
        )
        second.append(
            [
                pltpu.make_async_copy(
                    ref.at[:, k], downs.at[q, pl.ds(i * width, width)], in_sems.at[q, 4 + i]
                )
                for i, ref in enumerate((down_ref, down2_ref))
            ]
        )
    for group in first + second:
        for copy in group:
            copy.start()
    arrival.wait()
    total = None
    for q in range(QUARTERS):
        at = mains + q * TAIL
        rows = jnp.concatenate(
            [slots[chip, q * MAIN : (q + 1) * MAIN] for chip in range(chips)]
            + [slots[chip, at : at + TAIL] for chip in range(chips)],
            axis=0,
        )
        for copy in first[q]:
            copy.wait()
        added = jnp.dot(rows, ins[q], preferred_element_type=jnp.float32)
        total = added if total is None else total + added
    gate = total[:, : 2 * width]
    hidden = (gate * jax.nn.sigmoid(gate) * total[:, 2 * width :]).astype(jnp.bfloat16)
    for q in range(QUARTERS):
        at = mains + q * TAIL
        for copy in second[q]:
            copy.wait()
        partial = jnp.dot(hidden, downs[q], preferred_element_type=jnp.float32).astype(
            jnp.bfloat16
        )
        for chip in range(chips):
            outs[chip, q * MAIN : (q + 1) * MAIN] = partial[chip * MAIN : (chip + 1) * MAIN]
            tail = chips * MAIN + chip * TAIL
            outs[chip, at : at + TAIL] = partial[tail : tail + TAIL]
    copies = [
        pltpu.make_async_copy(outs.at[chip], out_ref.at[chip], out_sems.at[chip])
        for chip in range(chips)
    ]
    for copy in copies:
        copy.start()
    for copy in copies:
        copy.wait()


def ffn(slots, *weights):
    model, width = weights[0].shape
    chips = slots.shape[0]
    quarter = model // QUARTERS
    hbm = pl.BlockSpec(memory_space=pltpu.HBM)
    return pl.pallas_call(
        ffn_kernel,
        in_specs=[hbm] * 7,
        out_specs=hbm,
        out_shape=jax.ShapeDtypeStruct(slots.shape, jnp.bfloat16),
        scratch_shapes=[
            pltpu.VMEM(slots.shape, jnp.bfloat16),
            pltpu.VMEM((QUARTERS, quarter, 4 * width), jnp.bfloat16),
            pltpu.VMEM((QUARTERS, 2 * width, quarter), jnp.bfloat16),
            pltpu.VMEM(slots.shape, jnp.bfloat16),
            pltpu.SemaphoreType.DMA,
            pltpu.SemaphoreType.DMA((QUARTERS, 6)),
            pltpu.SemaphoreType.DMA((chips,)),
        ],
        cost_estimate=cost(2 * chips * CAP * model * width * 6, 14000000),
        compiler_params=pltpu.CompilerParams(vmem_limit_bytes=60 << 20),
        name="ffn",
    )(slots, *weights)


def combine_kernel(mix_ref, back_ref, out_ref):
    blocks, count, depth = out_ref.shape
    per_quarter = blocks // QUARTERS
    summed = lax.dot_general(
        mix_ref[...], back_ref[...], (((0,), (0,)), ((), ())), preferred_element_type=jnp.float32
    ).astype(jnp.bfloat16)
    for q in range(QUARTERS):
        for s in range(per_quarter):
            out_ref[q * per_quarter + s] = summed[
                q * count : (q + 1) * count, s * depth : (s + 1) * depth
            ]


def combine(mix, back, count, blocks):
    rows, quarter = back.shape
    depth = QUARTERS * quarter // blocks
    return pl.pallas_call(
        combine_kernel,
        out_shape=jax.ShapeDtypeStruct((blocks, count, depth), jnp.bfloat16),
        cost_estimate=cost(2 * rows * quarter * 128, 2400000),
        compiler_params=pltpu.CompilerParams(vmem_limit_bytes=12 << 20),
        name="combine",
    )(mix, back)


def on_device(tokens, expert_ids, route_logits, gate_weight, up_weight, down_weight):
    chips = lax.axis_size("x")
    parts = lax.axis_size("tp")
    count, depth = tokens.shape
    swap = [(0, 1), (1, 0)]
    ids = expert_ids.T
    gathered = lax.all_gather(tokens, "tp")
    outgoing = dispatch(ids, gathered, chips)
    gate, up, down, outgoing = lax.optimization_barrier(
        (gate_weight, up_weight, down_weight, outgoing)
    )
    incoming = lax.all_to_all(outgoing, "x", 0, 0, tiled=True)
    gate2 = lax.ppermute(gate, "core", swap)
    up2 = lax.ppermute(up, "core", swap)
    down2 = lax.ppermute(down, "core", swap)
    partial_value = ffn(incoming, gate, gate2, up, up2, down, down2)
    returned = lax.all_to_all(partial_value, "x", 0, 0, tiled=True)
    mix = mixing(ids, route_logits.T, chips)
    back = returned.reshape(chips * QUARTERS * CAP, parts * depth // QUARTERS)
    combined = combine(mix, back, count, parts)
    blocks = lax.all_to_all(combined, "tp", 0, 0, tiled=True)
    return jnp.sum(blocks.astype(jnp.float32), axis=0).astype(jnp.bfloat16)


def solution(mesh):
    sizes = [mesh.shape[axis] for axis in ("rep", "exp", "tp")]
    devices = mesh.devices.reshape(sizes[0], sizes[1] // CORES, CORES, sizes[2])
    split = Mesh(devices, ("rep", "x", "core", "tp"))
    tokens = ("rep", "x", "core")
    hidden = ("x", "core", "tp")
    return jax.shard_map(
        on_device,
        mesh=split,
        in_specs=(
            P(tokens, "tp"),
            P(tokens, None),
            P(tokens, None),
            P(None, hidden),
            P(None, hidden),
            P(hidden, None),
        ),
        out_specs=P(tokens, "tp"),
        check_vma=False,
    )
```

```python
import functools

import jax
import jax.numpy as jnp
from jax import lax
from jax.experimental import pallas as pl
from jax.experimental.pallas import tpu as pltpu
from jax.sharding import Mesh, PartitionSpec as P


EXPERTS = 4
CAP = 20
MAIN = 16
TAIL = CAP - MAIN
QUARTERS = 4
CORES = 2


def cost(flops, nbytes):
    return pl.CostEstimate(flops=flops, bytes_accessed=nbytes, transcendentals=0)


def count_at_least(index, width, parts):
    total = jnp.zeros_like(index)
    for k in range(1, parts):
        total = total + (index >= k * width).astype(jnp.int32)
    return total


def placed(ids, expert, slot, before):
    chosen = ((ids[0:1, :] == expert) | (ids[1:2, :] == expert)).astype(jnp.float32)
    position = jnp.dot(chosen, before, preferred_element_type=jnp.float32)
    return chosen * (position == slot.astype(jnp.float32)).astype(jnp.float32)


def grouped(row, groups):
    later = row >= groups * MAIN
    rest = row - groups * MAIN
    main = count_at_least(row, MAIN, groups)
    tail = count_at_least(rest, TAIL, groups)
    group = jnp.where(later, tail, main)
    slot = jnp.where(later, MAIN + rest - TAIL * tail, row - MAIN * main)
    return group, slot


def dispatch_kernel(chips, ids_ref, tokens_ref, out_ref):
    count = tokens_ref.shape[0]
    row = lax.broadcasted_iota(jnp.int32, (EXPERTS * CAP, count), 0)
    expert = count_at_least(row, CAP, EXPERTS)
    slot = row - CAP * expert
    first = lax.broadcasted_iota(jnp.int32, (count, count), 0)
    second = lax.broadcasted_iota(jnp.int32, (count, count), 1)
    before = (first < second).astype(jnp.float32)
    placement = placed(ids_ref[...], expert, slot, before).astype(jnp.bfloat16)
    slots = jnp.dot(placement, tokens_ref[...], preferred_element_type=jnp.float32).astype(
        jnp.bfloat16
    )
    per_expert = chips // EXPERTS
    for chip in range(chips):
        e = chip // per_expert
        out_ref[chip] = slots[e * CAP : (e + 1) * CAP]


def dispatch(ids, tokens, chips):
    count, features = tokens.shape
    return pl.pallas_call(
        functools.partial(dispatch_kernel, chips),
        out_shape=jax.ShapeDtypeStruct((chips, CAP, features), jnp.bfloat16),
        cost_estimate=cost(2 * EXPERTS * CAP * count * features, 200000),
        compiler_params=pltpu.CompilerParams(vmem_limit_bytes=4 << 20),
        name="dispatch",
    )(ids, tokens)


def gather_rows_kernel(in_ref, out_ref):
    chips = in_ref.shape[0]
    for chip in range(chips):
        out_ref[chip * MAIN : (chip + 1) * MAIN] = in_ref[chip, :MAIN]
        at = chips * MAIN + chip * TAIL
        out_ref[at : at + TAIL] = in_ref[chip, MAIN:]


def gather_rows(slots):
    chips, _, depth = slots.shape
    return pl.pallas_call(
        gather_rows_kernel,
        out_shape=jax.ShapeDtypeStruct((chips * CAP, depth), jnp.bfloat16),
        cost_estimate=cost(1000, 250000),
        compiler_params=pltpu.CompilerParams(vmem_limit_bytes=4 << 20),
        name="gather_rows",
    )(slots)


def mixing_kernel(chips, count, ids_ref, logits_ref, out_ref):
    lanes = ids_ref.shape[1]
    rows = chips * QUARTERS * CAP
    row = lax.broadcasted_iota(jnp.int32, (rows, lanes), 0)
    chip = count_at_least(row, QUARTERS * CAP, chips)
    quarter, slot = grouped(row - QUARTERS * CAP * chip, QUARTERS)
    expert = count_at_least(chip, chips // EXPERTS, EXPERTS)
    lane = lax.broadcasted_iota(jnp.int32, (rows, lanes), 1)
    own = (count_at_least(lane, count, QUARTERS) == quarter).astype(jnp.float32)
    first = lax.broadcasted_iota(jnp.int32, (lanes, lanes), 0)
    second = lax.broadcasted_iota(jnp.int32, (lanes, lanes), 1)
    same = count_at_least(first, count, QUARTERS) == count_at_least(second, count, QUARTERS)
    before = ((first < second) & same).astype(jnp.float32)
    ids = ids_ref[...]
    diff = logits_ref[0:1, :] - logits_ref[1:2, :]
    share = jnp.where(ids[0:1, :] == expert, jax.nn.sigmoid(diff), jax.nn.sigmoid(-diff))
    out_ref[...] = (placed(ids, expert, slot, before) * share * own).astype(jnp.bfloat16)


def mixing(ids, logits, chips):
    count = ids.shape[1]
    rows = chips * QUARTERS * CAP
    return pl.pallas_call(
        functools.partial(mixing_kernel, chips, count),
        out_shape=jax.ShapeDtypeStruct((rows, QUARTERS * count), jnp.bfloat16),
        cost_estimate=cost(2 * rows * 128 * 128, 200000),
        compiler_params=pltpu.CompilerParams(vmem_limit_bytes=8 << 20),
        name="mixing",
    )(jnp.tile(ids, (1, QUARTERS)), jnp.tile(logits, (1, QUARTERS)))


def multiply(total, tokens, first, weights, start, number):
    for b in range(0, number, 2):
        rows = jnp.concatenate([tokens[first + b], tokens[first + b + 1]], axis=1)
        weight = jnp.concatenate([weights[start + b], weights[start + b + 1]], axis=0)
        added = jnp.dot(rows, weight, preferred_element_type=jnp.float32)
        total = added if total is None else total + added
    return total


def own_kernel(slots_ref, gate_ref, gate2_ref, up_ref, up2_ref, out_ref, ins, sems):
    pairs = slots_ref.shape[0]
    parity = lax.axis_index("odd")
    width = gate_ref.shape[-1]
    half = pairs // 2
    refs = (gate_ref, gate2_ref, up_ref, up2_ref)
    groups = [
        [
            pltpu.make_async_copy(
                ref.at[pl.ds(g * half, half), parity],
                ins.at[pl.ds(g * half, half), :, pl.ds(i * width, width)],
                sems.at[g, i],
            )
            for i, ref in enumerate(refs)
        ]
        for g in range(2)
    ]
    for group in groups:
        for copy in group:
            copy.start()
    total = None
    for g, group in enumerate(groups):
        for copy in group:
            copy.wait()
        total = multiply(total, slots_ref, g * half, ins, g * half, half)
    out_ref[...] = total


def own_part(slots, *weights):
    pairs, rows, depth = slots.shape
    width = weights[0].shape[-1]
    hbm = pl.BlockSpec(memory_space=pltpu.HBM)
    return pl.pallas_call(
        own_kernel,
        in_specs=[pl.BlockSpec(memory_space=pltpu.VMEM)] + [hbm] * 4,
        out_specs=pl.BlockSpec(memory_space=pltpu.VMEM),
        out_shape=jax.ShapeDtypeStruct((rows, 4 * width), jnp.float32),
        scratch_shapes=[
            pltpu.VMEM((pairs, depth, 4 * width), jnp.bfloat16),
            pltpu.SemaphoreType.DMA((2, 4)),
        ],
        cost_estimate=cost(2 * pairs * rows * depth * 4 * width, 4200000),
        compiler_params=pltpu.CompilerParams(vmem_limit_bytes=60 << 20),
        name="own_part",
    )(slots, *weights)


def ffn_kernel(
    total_ref, left_ref, right_ref, gate_ref, gate2_ref, up_ref, up2_ref, down_ref, down2_ref, out_ref, ins, downs, outs, in_sems, down_sems, out_sems
):
    half = left_ref.shape[0]
    chips, _, quarter = out_ref.shape
    parity = 1 - lax.axis_index("odd")
    width = gate_ref.shape[-1]
    refs = (gate_ref, gate2_ref, up_ref, up2_ref)
    groups = [
        [
            pltpu.make_async_copy(
                ref.at[pl.ds(g * half, half), parity],
                ins.at[pl.ds(g * half, half), :, pl.ds(i * width, width)],
                in_sems.at[g, i],
            )
            for i, ref in enumerate(refs)
        ]
        for g in range(2)
    ]
    second = [
        [
            pltpu.make_async_copy(
                ref.at[:, pl.ds(q * quarter, quarter)],
                downs.at[q, pl.ds(i * width, width)],
                down_sems.at[q, i],
            )
            for i, ref in enumerate((down_ref, down2_ref))
        ]
        for q in range(QUARTERS)
    ]
    for group in groups + second:
        for copy in group:
            copy.start()
    total = total_ref[...]
    for g, group in enumerate(groups):
        for copy in group:
            copy.wait()
        total = multiply(total, (left_ref, right_ref)[g], 0, ins, g * half, half)
    gate = total[:, : 2 * width]
    hidden = (gate * jax.nn.sigmoid(gate) * total[:, 2 * width :]).astype(jnp.bfloat16)
    for q in range(QUARTERS):
        at = QUARTERS * MAIN + q * TAIL
        for copy in second[q]:
            copy.wait()
        partial = jnp.dot(hidden, downs[q], preferred_element_type=jnp.float32).astype(
            jnp.bfloat16
        )
        for chip in range(chips):
            outs[chip, q * MAIN : (q + 1) * MAIN] = partial[chip * MAIN : (chip + 1) * MAIN]
            tail = chips * MAIN + chip * TAIL
            outs[chip, at : at + TAIL] = partial[tail : tail + TAIL]
    copies = [
        pltpu.make_async_copy(outs.at[chip], out_ref.at[chip], out_sems.at[chip])
        for chip in range(chips)
    ]
    for copy in copies:
        copy.start()
    for copy in copies:
        copy.wait()


def ffn(total, left, right, chips, *weights):
    half, rows, depth = left.shape
    width, model = weights[-1].shape
    quarter = model // QUARTERS
    hbm = pl.BlockSpec(memory_space=pltpu.HBM)
    vmem = pl.BlockSpec(memory_space=pltpu.VMEM)
    out = (chips, QUARTERS * CAP, quarter)
    return pl.pallas_call(
        ffn_kernel,
        in_specs=[vmem] * 3 + [hbm] * 6,
        out_specs=hbm,
        out_shape=jax.ShapeDtypeStruct(out, jnp.bfloat16),
        scratch_shapes=[
            pltpu.VMEM((2 * half, depth, 4 * width), jnp.bfloat16),
            pltpu.VMEM((QUARTERS, 2 * width, quarter), jnp.bfloat16),
            pltpu.VMEM(out, jnp.bfloat16),
            pltpu.SemaphoreType.DMA((2, 4)),
            pltpu.SemaphoreType.DMA((QUARTERS, 2)),
            pltpu.SemaphoreType.DMA((chips,)),
        ],
        cost_estimate=cost(2 * rows * model * width * 4, 9000000),
        compiler_params=pltpu.CompilerParams(vmem_limit_bytes=60 << 20),
        name="ffn",
    )(total, left, right, *weights)


def combine_kernel(mix_ref, back_ref, out_ref):
    blocks, count, depth = out_ref.shape
    per_quarter = blocks // QUARTERS
    summed = lax.dot_general(
        mix_ref[...], back_ref[...], (((0,), (0,)), ((), ())), preferred_element_type=jnp.float32
    ).astype(jnp.bfloat16)
    for q in range(QUARTERS):
        for s in range(per_quarter):
            out_ref[q * per_quarter + s] = summed[
                q * count : (q + 1) * count, s * depth : (s + 1) * depth
            ]


def combine(mix, back, count, blocks):
    rows, quarter = back.shape
    depth = QUARTERS * quarter // blocks
    return pl.pallas_call(
        combine_kernel,
        out_shape=jax.ShapeDtypeStruct((blocks, count, depth), jnp.bfloat16),
        cost_estimate=cost(2 * rows * quarter * 128, 2400000),
        compiler_params=pltpu.CompilerParams(vmem_limit_bytes=12 << 20),
        name="combine",
    )(mix, back)


def on_device(tokens, expert_ids, route_logits, gate_weight, up_weight, down_weight):
    chips = lax.axis_size("x")
    pairs = lax.axis_size("pair")
    parts = 2 * pairs
    count, depth = tokens.shape
    swap = [(0, 1), (1, 0)]
    along = ("pair", "odd")
    ids = expert_ids.T
    outgoing = dispatch(ids, tokens, chips)
    incoming = lax.all_to_all(outgoing, "x", 0, 0, tiled=True)
    own = lax.all_gather(gather_rows(incoming), "pair")
    gate, up, down, own = lax.optimization_barrier((gate_weight, up_weight, down_weight, own))
    up_z = [(i, (i + 1) % parts) for i in range(parts)]
    down_z = [((i + 1) % parts, i) for i in range(parts)]
    left = lax.ppermute(own[: pairs // 2], along, up_z)
    right = lax.ppermute(own[pairs // 2 :], along, down_z)
    gate2 = lax.ppermute(gate, "core", swap)
    up2 = lax.ppermute(up, "core", swap)
    down2 = lax.ppermute(down, "core", swap)
    blocks = [w.reshape(pairs, 2, depth, w.shape[1]) for w in (gate, gate2, up, up2)]
    total = own_part(own, *blocks)
    partial_value = ffn(total, left, right, chips, *blocks, down, down2)
    returned = lax.all_to_all(partial_value, "x", 0, 0, tiled=True)
    mix = mixing(ids, route_logits.T, chips)
    back = returned.reshape(chips * QUARTERS * CAP, parts * depth // QUARTERS)
    combined = combine(mix, back, count, parts)
    blocks = lax.all_to_all(combined, along, 0, 0, tiled=True)
    return jnp.sum(blocks.astype(jnp.float32), axis=0).astype(jnp.bfloat16)


def solution(mesh):
    sizes = [mesh.shape[axis] for axis in ("rep", "exp", "tp")]
    devices = mesh.devices.reshape(sizes[0], sizes[1] // CORES, CORES, sizes[2] // 2, 2)
    split = Mesh(devices, ("rep", "x", "core", "pair", "odd"))
    tokens = ("rep", "x", "core")
    features = ("pair", "odd")
    hidden = ("x", "core", "pair", "odd")
    return jax.shard_map(
        on_device,
        mesh=split,
        in_specs=(
            P(tokens, features),
            P(tokens, None),
            P(tokens, None),
            P(None, hidden),
            P(None, hidden),
            P(hidden, None),
        ),
        out_specs=P(tokens, features),
        check_vma=False,
    )
```

```python
import functools

import jax
import jax.numpy as jnp
from jax import lax
from jax.experimental import pallas as pl
from jax.experimental.pallas import tpu as pltpu
from jax.sharding import Mesh, PartitionSpec as P


EXPERTS = 4
CAP = 20
MAIN = 16
TAIL = CAP - MAIN
QUARTERS = 4
CORES = 2


def cost(flops, nbytes):
    return pl.CostEstimate(flops=flops, bytes_accessed=nbytes, transcendentals=0)


def count_at_least(index, width, parts):
    total = jnp.zeros_like(index)
    for k in range(1, parts):
        total = total + (index >= k * width).astype(jnp.int32)
    return total


def placed(ids, expert, slot, before):
    chosen = ((ids[0:1, :] == expert) | (ids[1:2, :] == expert)).astype(jnp.float32)
    position = jnp.dot(chosen, before, preferred_element_type=jnp.float32)
    return chosen * (position == slot.astype(jnp.float32)).astype(jnp.float32)


def grouped(row, groups):
    later = row >= groups * MAIN
    rest = row - groups * MAIN
    main = count_at_least(row, MAIN, groups)
    tail = count_at_least(rest, TAIL, groups)
    group = jnp.where(later, tail, main)
    slot = jnp.where(later, MAIN + rest - TAIL * tail, row - MAIN * main)
    return group, slot


def dispatch_kernel(chips, ids_ref, tokens_ref, out_ref):
    count = tokens_ref.shape[0]
    row = lax.broadcasted_iota(jnp.int32, (EXPERTS * CAP, count), 0)
    expert = count_at_least(row, CAP, EXPERTS)
    slot = row - CAP * expert
    first = lax.broadcasted_iota(jnp.int32, (count, count), 0)
    second = lax.broadcasted_iota(jnp.int32, (count, count), 1)
    before = (first < second).astype(jnp.float32)
    placement = placed(ids_ref[...], expert, slot, before).astype(jnp.bfloat16)
    slots = jnp.dot(placement, tokens_ref[...], preferred_element_type=jnp.float32).astype(
        jnp.bfloat16
    )
    per_expert = chips // EXPERTS
    for chip in range(chips):
        e = chip // per_expert
        out_ref[chip] = slots[e * CAP : (e + 1) * CAP]


def dispatch(ids, tokens, chips):
    count, features = tokens.shape
    return pl.pallas_call(
        functools.partial(dispatch_kernel, chips),
        out_shape=jax.ShapeDtypeStruct((chips, CAP, features), jnp.bfloat16),
        cost_estimate=cost(2 * EXPERTS * CAP * count * features, 200000),
        compiler_params=pltpu.CompilerParams(vmem_limit_bytes=4 << 20),
        name="dispatch",
    )(ids, tokens)


def gather_rows_kernel(in_ref, out_ref):
    chips = in_ref.shape[0]
    for chip in range(chips):
        out_ref[chip * MAIN : (chip + 1) * MAIN] = in_ref[chip, :MAIN]
        at = chips * MAIN + chip * TAIL
        out_ref[at : at + TAIL] = in_ref[chip, MAIN:]


def gather_rows(slots):
    chips, _, depth = slots.shape
    return pl.pallas_call(
        gather_rows_kernel,
        out_shape=jax.ShapeDtypeStruct((chips * CAP, depth), jnp.bfloat16),
        cost_estimate=cost(1000, 250000),
        compiler_params=pltpu.CompilerParams(vmem_limit_bytes=4 << 20),
        name="gather_rows",
    )(slots)


def mixing_kernel(chips, count, ids_ref, logits_ref, out_ref):
    lanes = ids_ref.shape[1]
    rows = chips * QUARTERS * CAP
    row = lax.broadcasted_iota(jnp.int32, (rows, lanes), 0)
    chip = count_at_least(row, QUARTERS * CAP, chips)
    quarter, slot = grouped(row - QUARTERS * CAP * chip, QUARTERS)
    expert = count_at_least(chip, chips // EXPERTS, EXPERTS)
    lane = lax.broadcasted_iota(jnp.int32, (rows, lanes), 1)
    own = (count_at_least(lane, count, QUARTERS) == quarter).astype(jnp.float32)
    first = lax.broadcasted_iota(jnp.int32, (lanes, lanes), 0)
    second = lax.broadcasted_iota(jnp.int32, (lanes, lanes), 1)
    same = count_at_least(first, count, QUARTERS) == count_at_least(second, count, QUARTERS)
    before = ((first < second) & same).astype(jnp.float32)
    ids = ids_ref[...]
    diff = logits_ref[0:1, :] - logits_ref[1:2, :]
    share = jnp.where(ids[0:1, :] == expert, jax.nn.sigmoid(diff), jax.nn.sigmoid(-diff))
    out_ref[...] = (placed(ids, expert, slot, before) * share * own).astype(jnp.bfloat16)


def mixing(ids, logits, chips):
    count = ids.shape[1]
    rows = chips * QUARTERS * CAP
    return pl.pallas_call(
        functools.partial(mixing_kernel, chips, count),
        out_shape=jax.ShapeDtypeStruct((rows, QUARTERS * count), jnp.bfloat16),
        cost_estimate=cost(2 * rows * 128 * 128, 200000),
        compiler_params=pltpu.CompilerParams(vmem_limit_bytes=8 << 20),
        name="mixing",
    )(jnp.tile(ids, (1, QUARTERS)), jnp.tile(logits, (1, QUARTERS)))


def multiply(total, tokens, first, weights, start, number):
    for b in range(0, number, 2):
        rows = jnp.concatenate([tokens[first + b], tokens[first + b + 1]], axis=1)
        weight = jnp.concatenate([weights[start + b], weights[start + b + 1]], axis=0)
        added = jnp.dot(rows, weight, preferred_element_type=jnp.float32)
        total = added if total is None else total + added
    return total


def own_kernel(slots_ref, gate_ref, gate2_ref, up_ref, up2_ref, out_ref, ins, sems):
    pairs = slots_ref.shape[0]
    parity = lax.axis_index("odd")
    width = gate_ref.shape[-1]
    half = pairs // 2
    refs = (gate_ref, gate2_ref, up_ref, up2_ref)
    groups = [
        [
            pltpu.make_async_copy(
                ref.at[pl.ds(g * half, half), parity],
                ins.at[pl.ds(g * half, half), :, pl.ds(i * width, width)],
                sems.at[g, i],
            )
            for i, ref in enumerate(refs)
        ]
        for g in range(2)
    ]
    for group in groups:
        for copy in group:
            copy.start()
    total = None
    for g, group in enumerate(groups):
        for copy in group:
            copy.wait()
        total = multiply(total, slots_ref, g * half, ins, g * half, half)
    out_ref[...] = total


def own_part(slots, *weights):
    pairs, rows, depth = slots.shape
    width = weights[0].shape[-1]
    hbm = pl.BlockSpec(memory_space=pltpu.HBM)
    return pl.pallas_call(
        own_kernel,
        in_specs=[pl.BlockSpec(memory_space=pltpu.VMEM)] + [hbm] * 4,
        out_specs=pl.BlockSpec(memory_space=pltpu.VMEM),
        out_shape=jax.ShapeDtypeStruct((rows, 4 * width), jnp.float32),
        scratch_shapes=[
            pltpu.VMEM((pairs, depth, 4 * width), jnp.bfloat16),
            pltpu.SemaphoreType.DMA((2, 4)),
        ],
        cost_estimate=cost(2 * pairs * rows * depth * 4 * width, 4200000),
        compiler_params=pltpu.CompilerParams(vmem_limit_bytes=60 << 20),
        name="own_part",
    )(slots, *weights)


def down_copies(refs, scratch, sems, parity):
    pairs, _, depth = scratch.shape
    width = refs[0].shape[0]
    return [
        [
            pltpu.make_async_copy(
                ref.at[:, pl.ds(pl.multiple_of((2 * b + parity) * depth, 128), depth)],
                scratch.at[b, pl.ds(i * width, width)],
                sems.at[b, i],
            )
            for i, ref in enumerate(refs)
        ]
        for b in range(pairs)
    ]


def down_pair(hidden, scratch, copies, b):
    for copy in copies[b] + copies[b + 1]:
        copy.wait()
    weight = jnp.concatenate([scratch[b], scratch[b + 1]], axis=1)
    return jnp.dot(hidden, weight, preferred_element_type=jnp.float32)


def ffn_kernel(
    total_ref, left_ref, right_ref, gate_ref, gate2_ref, up_ref, up2_ref, down_ref, down2_ref, hidden_ref, to_right_ref, to_left_ref, ins, downs, in_sems, down_sems
):
    half, _, depth = left_ref.shape
    parity = 1 - lax.axis_index("odd")
    width = gate_ref.shape[-1]
    refs = (gate_ref, gate2_ref, up_ref, up2_ref)
    groups = [
        [
            pltpu.make_async_copy(
                ref.at[pl.ds(g * half, half), parity],
                ins.at[pl.ds(g * half, half), :, pl.ds(i * width, width)],
                in_sems.at[g, i],
            )
            for i, ref in enumerate(refs)
        ]
        for g in range(2)
    ]
    second = down_copies((down_ref, down2_ref), downs, down_sems, parity)
    for group in groups + second:
        for copy in group:
            copy.start()
    total = total_ref[...]
    for g, group in enumerate(groups):
        for copy in group:
            copy.wait()
        total = multiply(total, (left_ref, right_ref)[g], 0, ins, g * half, half)
    gate = total[:, : 2 * width]
    hidden = (gate * jax.nn.sigmoid(gate) * total[:, 2 * width :]).astype(jnp.bfloat16)
    hidden_ref[...] = hidden
    for b in range(0, 2 * half, 2):
        partial = down_pair(hidden, downs, second, b).astype(jnp.bfloat16)
        out_ref, at = (to_right_ref, b) if b < half else (to_left_ref, b - half)
        out_ref[at] = partial[:, :depth]
        out_ref[at + 1] = partial[:, depth:]


def ffn(total, left, right, *weights):
    half, rows, depth = left.shape
    width, model = weights[-1].shape
    hbm = pl.BlockSpec(memory_space=pltpu.HBM)
    vmem = pl.BlockSpec(memory_space=pltpu.VMEM)
    sent = jax.ShapeDtypeStruct(left.shape, jnp.bfloat16)
    return pl.pallas_call(
        ffn_kernel,
        in_specs=[vmem] * 3 + [hbm] * 6,
        out_specs=(vmem, vmem, vmem),
        out_shape=(jax.ShapeDtypeStruct((rows, 2 * width), jnp.bfloat16), sent, sent),
        scratch_shapes=[
            pltpu.VMEM((2 * half, depth, 4 * width), jnp.bfloat16),
            pltpu.VMEM((2 * half, 2 * width, depth), jnp.bfloat16),
            pltpu.SemaphoreType.DMA((2, 4)),
            pltpu.SemaphoreType.DMA((2 * half, 2)),
        ],
        cost_estimate=cost(2 * rows * model * width * 3, 7000000),
        compiler_params=pltpu.CompilerParams(vmem_limit_bytes=60 << 20),
        name="ffn",
    )(total, left, right, *weights)


def own_down_kernel(hidden_ref, down_ref, down2_ref, out_ref):
    pairs, _, depth = out_ref.shape
    parity = lax.axis_index("odd")

    def block(b):
        lanes = pl.ds(pl.multiple_of((2 * b + parity) * depth, 128), depth)
        return jnp.concatenate([down_ref[:, lanes], down2_ref[:, lanes]], axis=0)

    for b in range(0, pairs, 2):
        weight = jnp.concatenate([block(b), block(b + 1)], axis=1)
        partial = jnp.dot(hidden_ref[...], weight, preferred_element_type=jnp.float32)
        out_ref[b] = partial[:, :depth]
        out_ref[b + 1] = partial[:, depth:]


def own_down(hidden, down, down2, pairs):
    rows = hidden.shape[0]
    width, model = down.shape
    depth = model // (2 * pairs)
    return pl.pallas_call(
        own_down_kernel,
        out_shape=jax.ShapeDtypeStruct((pairs, rows, depth), jnp.float32),
        cost_estimate=cost(2 * rows * model * width, 4000000),
        compiler_params=pltpu.CompilerParams(vmem_limit_bytes=16 << 20),
        name="own_down",
    )(hidden, down, down2)


def join_kernel(own_ref, left_ref, right_ref, out_ref):
    pairs, _, depth = own_ref.shape
    chips = out_ref.shape[0]
    half = pairs // 2
    per_quarter = pairs // QUARTERS
    for b in range(pairs):
        other = left_ref[b] if b < half else right_ref[b - half]
        both = (own_ref[b] + other.astype(jnp.float32)).astype(jnp.bfloat16)
        q, s = b // per_quarter, b % per_quarter
        at = QUARTERS * MAIN + q * TAIL
        lanes = slice(s * depth, (s + 1) * depth)
        for chip in range(chips):
            tail = chips * MAIN + chip * TAIL
            out_ref[chip, q * MAIN : (q + 1) * MAIN, lanes] = both[chip * MAIN : (chip + 1) * MAIN]
            out_ref[chip, at : at + TAIL, lanes] = both[tail : tail + TAIL]


def join(own, left, right, chips):
    pairs, rows, depth = own.shape
    out = (chips, QUARTERS * CAP, pairs * depth // QUARTERS)
    return pl.pallas_call(
        join_kernel,
        out_shape=jax.ShapeDtypeStruct(out, jnp.bfloat16),
        cost_estimate=cost(pairs * rows * depth, 8 * pairs * rows * depth),
        compiler_params=pltpu.CompilerParams(vmem_limit_bytes=16 << 20),
        name="join",
    )(own, left, right)


def combine_kernel(mix_ref, back_ref, out_ref):
    blocks, count, depth = out_ref.shape
    per_quarter = blocks // QUARTERS
    summed = lax.dot_general(
        mix_ref[...], back_ref[...], (((0,), (0,)), ((), ())), preferred_element_type=jnp.float32
    ).astype(jnp.bfloat16)
    for q in range(QUARTERS):
        for s in range(per_quarter):
            out_ref[q * per_quarter + s] = summed[
                q * count : (q + 1) * count, s * depth : (s + 1) * depth
            ]


def combine(mix, back, count, blocks):
    rows, quarter = back.shape
    depth = QUARTERS * quarter // blocks
    return pl.pallas_call(
        combine_kernel,
        out_shape=jax.ShapeDtypeStruct((blocks, count, depth), jnp.bfloat16),
        cost_estimate=cost(2 * rows * quarter * 128, 2400000),
        compiler_params=pltpu.CompilerParams(vmem_limit_bytes=12 << 20),
        name="combine",
    )(mix, back)


def on_device(tokens, expert_ids, route_logits, gate_weight, up_weight, down_weight):
    chips = lax.axis_size("x")
    pairs = lax.axis_size("pair")
    parts = 2 * pairs
    count, depth = tokens.shape
    swap = [(0, 1), (1, 0)]
    along = ("pair", "odd")
    ids = expert_ids.T
    up_z = [(i, (i + 1) % parts) for i in range(parts)]
    down_z = [((i + 1) % parts, i) for i in range(parts)]
    outgoing = dispatch(ids, tokens, chips)
    gate, up, down, outgoing = lax.optimization_barrier(
        (gate_weight, up_weight, down_weight, outgoing)
    )
    incoming = lax.all_to_all(outgoing, "x", 0, 0, tiled=True)
    gate2 = lax.ppermute(gate, "core", swap)
    up2 = lax.ppermute(up, "core", swap)
    down2 = lax.ppermute(down, "core", swap)
    own = lax.all_gather(gather_rows(incoming), "pair")
    left = lax.ppermute(own[: pairs // 2], along, up_z)
    right = lax.ppermute(own[pairs // 2 :], along, down_z)
    blocks = [w.reshape(pairs, 2, depth, w.shape[1]) for w in (gate, gate2, up, up2)]
    total = own_part(own, *blocks)
    hidden, to_right, to_left = ffn(total, left, right, *blocks, down, down2)
    from_left = lax.ppermute(to_right, along, up_z)
    from_right = lax.ppermute(to_left, along, down_z)
    partial_value = join(own_down(hidden, down, down2, pairs), from_left, from_right, chips)
    returned = lax.all_to_all(partial_value, "x", 0, 0, tiled=True)
    mix = mixing(ids, route_logits.T, chips)
    back = returned.reshape(chips * QUARTERS * CAP, pairs * depth // QUARTERS)
    combined = combine(mix, back, count, pairs)
    blocks = lax.all_to_all(combined, "pair", 0, 0, tiled=True)
    return jnp.sum(blocks.astype(jnp.float32), axis=0).astype(jnp.bfloat16)


def solution(mesh):
    sizes = [mesh.shape[axis] for axis in ("rep", "exp", "tp")]
    devices = mesh.devices.reshape(sizes[0], sizes[1] // CORES, CORES, sizes[2] // 2, 2)
    split = Mesh(devices, ("rep", "x", "core", "pair", "odd"))
    tokens = ("rep", "x", "core")
    features = ("pair", "odd")
    hidden = ("x", "core", "pair", "odd")
    return jax.shard_map(
        on_device,
        mesh=split,
        in_specs=(
            P(tokens, features),
            P(tokens, None),
            P(tokens, None),
            P(None, hidden),
            P(None, hidden),
            P(hidden, None),
        ),
        out_specs=P(tokens, features),
        check_vma=False,
    )
```

```python
import functools

import jax
import jax.numpy as jnp
from jax import lax
from jax.experimental import pallas as pl
from jax.experimental.pallas import tpu as pltpu
from jax.sharding import Mesh, PartitionSpec as P


EXPERTS = 4
CAP = 20
MAIN = 16
TAIL = CAP - MAIN
QUARTERS = 4
CORES = 2


def cost(flops, nbytes):
    return pl.CostEstimate(flops=flops, bytes_accessed=nbytes, transcendentals=0)


def count_at_least(index, width, parts):
    total = jnp.zeros_like(index)
    for k in range(1, parts):
        total = total + (index >= k * width).astype(jnp.int32)
    return total


def placed(ids, expert, slot, before):
    chosen = ((ids[0:1, :] == expert) | (ids[1:2, :] == expert)).astype(jnp.float32)
    position = jnp.dot(chosen, before, preferred_element_type=jnp.float32)
    return chosen * (position == slot.astype(jnp.float32)).astype(jnp.float32)


def grouped(row, groups):
    later = row >= groups * MAIN
    rest = row - groups * MAIN
    main = count_at_least(row, MAIN, groups)
    tail = count_at_least(rest, TAIL, groups)
    group = jnp.where(later, tail, main)
    slot = jnp.where(later, MAIN + rest - TAIL * tail, row - MAIN * main)
    return group, slot


def dispatch_kernel(chips, ids_ref, tokens_ref, out_ref):
    count = tokens_ref.shape[0]
    row = lax.broadcasted_iota(jnp.int32, (EXPERTS * CAP, count), 0)
    expert = count_at_least(row, CAP, EXPERTS)
    slot = row - CAP * expert
    first = lax.broadcasted_iota(jnp.int32, (count, count), 0)
    second = lax.broadcasted_iota(jnp.int32, (count, count), 1)
    before = (first < second).astype(jnp.float32)
    placement = placed(ids_ref[...], expert, slot, before).astype(jnp.bfloat16)
    slots = jnp.dot(placement, tokens_ref[...], preferred_element_type=jnp.float32).astype(
        jnp.bfloat16
    )
    per_expert = chips // EXPERTS
    for chip in range(chips):
        e = chip // per_expert
        out_ref[chip] = slots[e * CAP : (e + 1) * CAP]


def dispatch(ids, tokens, chips):
    count, features = tokens.shape
    return pl.pallas_call(
        functools.partial(dispatch_kernel, chips),
        out_shape=jax.ShapeDtypeStruct((chips, CAP, features), jnp.bfloat16),
        cost_estimate=cost(2 * EXPERTS * CAP * count * features, 200000),
        compiler_params=pltpu.CompilerParams(vmem_limit_bytes=60 << 20),
        name="dispatch",
    )(ids, tokens)


def gather_rows_kernel(in_ref, out_ref):
    chips = in_ref.shape[0]
    for chip in range(chips):
        out_ref[chip * MAIN : (chip + 1) * MAIN] = in_ref[chip, :MAIN]
        at = chips * MAIN + chip * TAIL
        out_ref[at : at + TAIL] = in_ref[chip, MAIN:]


def gather_rows(slots):
    chips, _, depth = slots.shape
    return pl.pallas_call(
        gather_rows_kernel,
        out_shape=jax.ShapeDtypeStruct((chips * CAP, depth), jnp.bfloat16),
        cost_estimate=cost(1000, 250000),
        compiler_params=pltpu.CompilerParams(vmem_limit_bytes=4 << 20),
        name="gather_rows",
    )(slots)


def mixing_kernel(chips, count, ids_ref, logits_ref, out_ref):
    lanes = ids_ref.shape[1]
    rows = chips * QUARTERS * CAP
    row = lax.broadcasted_iota(jnp.int32, (rows, lanes), 0)
    chip = count_at_least(row, QUARTERS * CAP, chips)
    quarter, slot = grouped(row - QUARTERS * CAP * chip, QUARTERS)
    expert = count_at_least(chip, chips // EXPERTS, EXPERTS)
    lane = lax.broadcasted_iota(jnp.int32, (rows, lanes), 1)
    own = (count_at_least(lane, count, QUARTERS) == quarter).astype(jnp.float32)
    first = lax.broadcasted_iota(jnp.int32, (lanes, lanes), 0)
    second = lax.broadcasted_iota(jnp.int32, (lanes, lanes), 1)
    same = count_at_least(first, count, QUARTERS) == count_at_least(second, count, QUARTERS)
    before = ((first < second) & same).astype(jnp.float32)
    ids = ids_ref[...]
    diff = logits_ref[0:1, :] - logits_ref[1:2, :]
    share = jnp.where(ids[0:1, :] == expert, jax.nn.sigmoid(diff), jax.nn.sigmoid(-diff))
    out_ref[...] = (placed(ids, expert, slot, before) * share * own).astype(jnp.bfloat16)


def mixing(ids, logits, chips):
    count = ids.shape[1]
    rows = chips * QUARTERS * CAP
    return pl.pallas_call(
        functools.partial(mixing_kernel, chips, count),
        out_shape=jax.ShapeDtypeStruct((rows, QUARTERS * count), jnp.bfloat16),
        cost_estimate=cost(2 * rows * 128 * 128, 200000),
        compiler_params=pltpu.CompilerParams(vmem_limit_bytes=8 << 20),
        name="mixing",
    )(jnp.tile(ids, (1, QUARTERS)), jnp.tile(logits, (1, QUARTERS)))


def side_by_side(refs, b, parity):
    return jnp.concatenate([ref[b, parity] for ref in refs], axis=1)


def multiply(total, tokens, refs, parity, start):
    for b in range(0, tokens.shape[0], 2):
        rows = jnp.concatenate([tokens[b], tokens[b + 1]], axis=1)
        weight = jnp.concatenate(
            [side_by_side(refs, start + b, parity), side_by_side(refs, start + b + 1, parity)],
            axis=0,
        )
        added = jnp.dot(rows, weight, preferred_element_type=jnp.float32)
        total = added if total is None else total + added
    return total


def own_kernel(slots_ref, gate_ref, gate2_ref, up_ref, up2_ref, out_ref):
    refs = (gate_ref, gate2_ref, up_ref, up2_ref)
    out_ref[...] = multiply(None, slots_ref, refs, lax.axis_index("odd"), 0)


def own_part(slots, *weights):
    pairs, rows, depth = slots.shape
    width = weights[0].shape[-1]
    return pl.pallas_call(
        own_kernel,
        out_shape=jax.ShapeDtypeStruct((rows, 4 * width), jnp.float32),
        cost_estimate=cost(2 * pairs * rows * depth * 4 * width, 4200000),
        compiler_params=pltpu.CompilerParams(vmem_limit_bytes=16 << 20),
        name="own_part",
    )(slots, *weights)


def down_pair(hidden, refs, b, parity, depth):
    def block(b):
        lanes = pl.ds(pl.multiple_of((2 * b + parity) * depth, 128), depth)
        return jnp.concatenate([ref[:, lanes] for ref in refs], axis=0)

    weight = jnp.concatenate([block(b), block(b + 1)], axis=1)
    return jnp.dot(hidden, weight, preferred_element_type=jnp.float32)


def ffn_kernel(
    total_ref, left_ref, right_ref, gate_ref, gate2_ref, up_ref, up2_ref, down_ref, down2_ref, hidden_ref, to_right_ref, to_left_ref
):
    half, _, depth = left_ref.shape
    parity = 1 - lax.axis_index("odd")
    width = gate_ref.shape[-1]
    refs = (gate_ref, gate2_ref, up_ref, up2_ref)
    total = multiply(total_ref[...], left_ref, refs, parity, 0)
    total = multiply(total, right_ref, refs, parity, half)
    gate = total[:, : 2 * width]
    hidden = (gate * jax.nn.sigmoid(gate) * total[:, 2 * width :]).astype(jnp.bfloat16)
    hidden_ref[...] = hidden
    for b in range(0, 2 * half, 2):
        partial = down_pair(hidden, (down_ref, down2_ref), b, parity, depth).astype(jnp.bfloat16)
        out_ref, at = (to_right_ref, b) if b < half else (to_left_ref, b - half)
        out_ref[at] = partial[:, :depth]
        out_ref[at + 1] = partial[:, depth:]


def ffn(total, left, right, *weights):
    _, rows, _ = left.shape
    width, model = weights[-1].shape
    sent = jax.ShapeDtypeStruct(left.shape, jnp.bfloat16)
    return pl.pallas_call(
        ffn_kernel,
        out_shape=(jax.ShapeDtypeStruct((rows, 2 * width), jnp.bfloat16), sent, sent),
        cost_estimate=cost(2 * rows * model * width * 3, 7000000),
        compiler_params=pltpu.CompilerParams(vmem_limit_bytes=20 << 20),
        name="ffn",
    )(total, left, right, *weights)


def own_down_kernel(hidden_ref, down_ref, down2_ref, out_ref):
    pairs, _, depth = out_ref.shape
    parity = lax.axis_index("odd")
    for b in range(0, pairs, 2):
        partial = down_pair(hidden_ref[...], (down_ref, down2_ref), b, parity, depth)
        out_ref[b] = partial[:, :depth]
        out_ref[b + 1] = partial[:, depth:]


def own_down(hidden, down, down2, pairs):
    rows = hidden.shape[0]
    width, model = down.shape
    depth = model // (2 * pairs)
    return pl.pallas_call(
        own_down_kernel,
        out_shape=jax.ShapeDtypeStruct((pairs, rows, depth), jnp.float32),
        cost_estimate=cost(2 * rows * model * width, 4000000),
        compiler_params=pltpu.CompilerParams(vmem_limit_bytes=16 << 20),
        name="own_down",
    )(hidden, down, down2)


def join_kernel(own_ref, left_ref, right_ref, out_ref):
    pairs, _, depth = own_ref.shape
    chips = out_ref.shape[0]
    half = pairs // 2
    per_quarter = pairs // QUARTERS
    for b in range(pairs):
        other = left_ref[b] if b < half else right_ref[b - half]
        both = (own_ref[b] + other.astype(jnp.float32)).astype(jnp.bfloat16)
        q, s = b // per_quarter, b % per_quarter
        at = QUARTERS * MAIN + q * TAIL
        lanes = slice(s * depth, (s + 1) * depth)
        for chip in range(chips):
            tail = chips * MAIN + chip * TAIL
            out_ref[chip, q * MAIN : (q + 1) * MAIN, lanes] = both[chip * MAIN : (chip + 1) * MAIN]
            out_ref[chip, at : at + TAIL, lanes] = both[tail : tail + TAIL]


def join(own, left, right, chips):
    pairs, rows, depth = own.shape
    out = (chips, QUARTERS * CAP, pairs * depth // QUARTERS)
    return pl.pallas_call(
        join_kernel,
        out_shape=jax.ShapeDtypeStruct(out, jnp.bfloat16),
        cost_estimate=cost(pairs * rows * depth, 8 * pairs * rows * depth),
        compiler_params=pltpu.CompilerParams(vmem_limit_bytes=16 << 20),
        name="join",
    )(own, left, right)


def combine_kernel(mix_ref, back_ref, out_ref):
    blocks, count, depth = out_ref.shape
    per_quarter = blocks // QUARTERS
    summed = lax.dot_general(
        mix_ref[...], back_ref[...], (((0,), (0,)), ((), ())), preferred_element_type=jnp.float32
    ).astype(jnp.bfloat16)
    for q in range(QUARTERS):
        for s in range(per_quarter):
            out_ref[q * per_quarter + s] = summed[
                q * count : (q + 1) * count, s * depth : (s + 1) * depth
            ]


def combine(mix, back, count, blocks):
    rows, quarter = back.shape
    depth = QUARTERS * quarter // blocks
    return pl.pallas_call(
        combine_kernel,
        out_shape=jax.ShapeDtypeStruct((blocks, count, depth), jnp.bfloat16),
        cost_estimate=cost(2 * rows * quarter * 128, 2400000),
        compiler_params=pltpu.CompilerParams(vmem_limit_bytes=12 << 20),
        name="combine",
    )(mix, back)


def on_device(tokens, expert_ids, route_logits, gate_weight, up_weight, down_weight):
    chips = lax.axis_size("x")
    pairs = lax.axis_size("pair")
    parts = 2 * pairs
    count, depth = tokens.shape
    swap = [(0, 1), (1, 0)]
    along = ("pair", "odd")
    ids = expert_ids.T
    up_z = [(i, (i + 1) % parts) for i in range(parts)]
    down_z = [((i + 1) % parts, i) for i in range(parts)]
    outgoing = dispatch(ids, tokens, chips)
    gate, up, down, outgoing = lax.optimization_barrier(
        (gate_weight, up_weight, down_weight, outgoing)
    )
    incoming = lax.all_to_all(outgoing, "x", 0, 0, tiled=True)
    gate2 = lax.ppermute(gate, "core", swap)
    up2 = lax.ppermute(up, "core", swap)
    down2 = lax.ppermute(down, "core", swap)
    own = lax.all_gather(gather_rows(incoming), "pair")
    left = lax.ppermute(own[: pairs // 2], along, up_z)
    right = lax.ppermute(own[pairs // 2 :], along, down_z)
    blocks = [w.reshape(pairs, 2, depth, w.shape[1]) for w in (gate, gate2, up, up2)]
    total = own_part(own, *blocks)
    hidden, to_right, to_left = ffn(total, left, right, *blocks, down, down2)
    from_left = lax.ppermute(to_right, along, up_z)
    from_right = lax.ppermute(to_left, along, down_z)
    partial_value = join(own_down(hidden, down, down2, pairs), from_left, from_right, chips)
    returned = lax.all_to_all(partial_value, "x", 0, 0, tiled=True)
    mix = mixing(ids, route_logits.T, chips)
    back = returned.reshape(chips * QUARTERS * CAP, pairs * depth // QUARTERS)
    combined = combine(mix, back, count, pairs)
    blocks = lax.all_to_all(combined, "pair", 0, 0, tiled=True)
    return jnp.sum(blocks.astype(jnp.float32), axis=0).astype(jnp.bfloat16)


def solution(mesh):
    sizes = [mesh.shape[axis] for axis in ("rep", "exp", "tp")]
    devices = mesh.devices.reshape(sizes[0], sizes[1] // CORES, CORES, sizes[2] // 2, 2)
    split = Mesh(devices, ("rep", "x", "core", "pair", "odd"))
    tokens = ("rep", "x", "core")
    features = ("pair", "odd")
    hidden = ("x", "core", "pair", "odd")
    return jax.shard_map(
        on_device,
        mesh=split,
        in_specs=(
            P(tokens, features),
            P(tokens, None),
            P(tokens, None),
            P(None, hidden),
            P(None, hidden),
            P(hidden, None),
        ),
        out_specs=P(tokens, features),
        check_vma=False,
    )
```

```python
import functools

import jax
import jax.numpy as jnp
from jax import lax
from jax.experimental import pallas as pl
from jax.experimental.pallas import tpu as pltpu
from jax.sharding import Mesh, PartitionSpec as P


EXPERTS = 4
CAP = 20
MAIN = 16
TAIL = CAP - MAIN
QUARTERS = 4
CLASSES = 4
CORES = 2


def cost(flops, nbytes):
    return pl.CostEstimate(flops=flops, bytes_accessed=nbytes, transcendentals=0)


def count_at_least(index, width, parts):
    total = jnp.zeros_like(index)
    for k in range(1, parts):
        total = total + (index >= k * width).astype(jnp.int32)
    return total


def placed(ids, expert, slot, before):
    chosen = ((ids[0:1, :] == expert) | (ids[1:2, :] == expert)).astype(jnp.float32)
    position = jnp.dot(chosen, before, preferred_element_type=jnp.float32)
    return chosen * (position == slot.astype(jnp.float32)).astype(jnp.float32)


def grouped(row, groups):
    later = row >= groups * MAIN
    rest = row - groups * MAIN
    main = count_at_least(row, MAIN, groups)
    tail = count_at_least(rest, TAIL, groups)
    group = jnp.where(later, tail, main)
    slot = jnp.where(later, MAIN + rest - TAIL * tail, row - MAIN * main)
    return group, slot


def dispatch_kernel(chips, ids_ref, tokens_ref, out_ref):
    blocks, count, _ = tokens_ref.shape
    per_expert = chips // EXPERTS
    row = lax.broadcasted_iota(jnp.int32, (EXPERTS * CAP, count), 0)
    expert, slot = grouped(row, EXPERTS)
    first = lax.broadcasted_iota(jnp.int32, (count, count), 0)
    second = lax.broadcasted_iota(jnp.int32, (count, count), 1)
    before = (first < second).astype(jnp.float32)
    placement = placed(ids_ref[...], expert, slot, before).astype(jnp.bfloat16)
    for q in range(blocks):
        slots = jnp.dot(placement, tokens_ref[q], preferred_element_type=jnp.float32).astype(
            jnp.bfloat16
        )
        for chip in range(chips):
            e = chip // per_expert
            out_ref[chip, q * MAIN : (q + 1) * MAIN] = slots[e * MAIN : (e + 1) * MAIN]
            to, at = QUARTERS * MAIN + q * TAIL, EXPERTS * MAIN + e * TAIL
            out_ref[chip, to : to + TAIL] = slots[at : at + TAIL]


def dispatch(ids, tokens, chips):
    blocks, count, depth = tokens.shape
    return pl.pallas_call(
        functools.partial(dispatch_kernel, chips),
        out_shape=jax.ShapeDtypeStruct((chips, blocks * CAP, depth), jnp.bfloat16),
        cost_estimate=cost(2 * EXPERTS * CAP * count * blocks * depth, 700000),
        compiler_params=pltpu.CompilerParams(vmem_limit_bytes=60 << 20),
        name="dispatch",
    )(ids, tokens)


def unpack_kernel(in_ref, out_ref, low_ref, high_ref):
    chips = in_ref.shape[0]
    for q in range(QUARTERS):
        at = QUARTERS * MAIN + q * TAIL
        rows = jnp.concatenate(
            [in_ref[chip, q * MAIN : (q + 1) * MAIN] for chip in range(chips)]
            + [in_ref[chip, at : at + TAIL] for chip in range(chips)],
            axis=0,
        )
        out_ref[q] = rows
        half_ref = low_ref if q < QUARTERS // 2 else high_ref
        half_ref[q % (QUARTERS // 2)] = rows


def unpack(slots):
    chips, _, depth = slots.shape
    half = jax.ShapeDtypeStruct((QUARTERS // 2, chips * CAP, depth), jnp.bfloat16)
    return pl.pallas_call(
        unpack_kernel,
        out_shape=(jax.ShapeDtypeStruct((QUARTERS, chips * CAP, depth), jnp.bfloat16), half, half),
        cost_estimate=cost(1000, 1500000),
        compiler_params=pltpu.CompilerParams(vmem_limit_bytes=8 << 20),
        name="unpack",
    )(slots)


def mixing_kernel(chips, count, ids_ref, logits_ref, out_ref):
    lanes = ids_ref.shape[1]
    rows = chips * QUARTERS * CAP
    row = lax.broadcasted_iota(jnp.int32, (rows, lanes), 0)
    chip = count_at_least(row, QUARTERS * CAP, chips)
    quarter, slot = grouped(row - QUARTERS * CAP * chip, QUARTERS)
    expert = count_at_least(chip, chips // EXPERTS, EXPERTS)
    lane = lax.broadcasted_iota(jnp.int32, (rows, lanes), 1)
    own = (count_at_least(lane, count, QUARTERS) == quarter).astype(jnp.float32)
    first = lax.broadcasted_iota(jnp.int32, (lanes, lanes), 0)
    second = lax.broadcasted_iota(jnp.int32, (lanes, lanes), 1)
    same = count_at_least(first, count, QUARTERS) == count_at_least(second, count, QUARTERS)
    before = ((first < second) & same).astype(jnp.float32)
    ids = ids_ref[...]
    diff = logits_ref[0:1, :] - logits_ref[1:2, :]
    share = jnp.where(ids[0:1, :] == expert, jax.nn.sigmoid(diff), jax.nn.sigmoid(-diff))
    out_ref[...] = (placed(ids, expert, slot, before) * share * own).astype(jnp.bfloat16)


def mixing(ids, logits, chips):
    count = ids.shape[1]
    rows = chips * QUARTERS * CAP
    return pl.pallas_call(
        functools.partial(mixing_kernel, chips, count),
        out_shape=jax.ShapeDtypeStruct((rows, QUARTERS * count), jnp.bfloat16),
        cost_estimate=cost(2 * rows * 128 * 128, 200000),
        compiler_params=pltpu.CompilerParams(vmem_limit_bytes=8 << 20),
        name="mixing",
    )(jnp.tile(ids, (1, QUARTERS)), jnp.tile(logits, (1, QUARTERS)))


def class_at(distance):
    return lax.rem(lax.axis_index("class") + CLASSES + distance, CLASSES)


def side_by_side(refs, q, kind):
    return jnp.concatenate([ref[q, kind] for ref in refs], axis=1)


def multiply(total, tokens, refs, kind, start):
    for b in range(0, tokens.shape[0], 2):
        rows = jnp.concatenate([tokens[b], tokens[b + 1]], axis=1)
        weight = jnp.concatenate(
            [side_by_side(refs, start + b, kind), side_by_side(refs, start + b + 1, kind)], axis=0
        )
        added = jnp.dot(rows, weight, preferred_element_type=jnp.float32)
        total = added if total is None else total + added
    return total


def own_kernel(slots_ref, gate_ref, gate2_ref, up_ref, up2_ref, out_ref):
    refs = (gate_ref, gate2_ref, up_ref, up2_ref)
    out_ref[...] = multiply(None, slots_ref, refs, class_at(0), 0)


def own_part(slots, *weights):
    blocks, rows, depth = slots.shape
    width = weights[0].shape[-1]
    return pl.pallas_call(
        own_kernel,
        out_shape=jax.ShapeDtypeStruct((rows, 4 * width), jnp.float32),
        cost_estimate=cost(2 * blocks * rows * depth * 4 * width, 2200000),
        compiler_params=pltpu.CompilerParams(vmem_limit_bytes=16 << 20),
        name="own_part",
    )(slots, *weights)


def down_pair(hidden, refs, q, kind, depth):
    def block(q):
        lanes = pl.ds(pl.multiple_of((CLASSES * q + kind) * depth, 128), depth)
        return jnp.concatenate([ref[:, lanes] for ref in refs], axis=0)

    weight = jnp.concatenate([block(q), block(q + 1)], axis=1)
    return jnp.dot(hidden, weight, preferred_element_type=jnp.float32)


def ffn_kernel(
    total_ref, left_ref, right_ref, left2_ref, right2_ref, gate_ref, gate2_ref, up_ref, up2_ref, down_ref, down2_ref, hidden_ref, to_right_ref, to_left_ref, to_right2_ref, to_left2_ref
):
    depth = left_ref.shape[2]
    width = gate_ref.shape[-1]
    half = QUARTERS // 2
    refs = (gate_ref, gate2_ref, up_ref, up2_ref)
    total = multiply(total_ref[...], left_ref, refs, class_at(-1), 0)
    total = multiply(total, right_ref, refs, class_at(1), 0)
    total = multiply(total, left2_ref, refs, class_at(2), 0)
    total = multiply(total, right2_ref, refs, class_at(2), half)
    gate = total[:, : 2 * width]
    hidden = (gate * jax.nn.sigmoid(gate) * total[:, 2 * width :]).astype(jnp.bfloat16)
    hidden_ref[...] = hidden
    downs = (down_ref, down2_ref)
    for out_ref, distance, start in (
        (to_right_ref, 1, 0),
        (to_left_ref, -1, 0),
        (to_right2_ref, 2, 0),
        (to_left2_ref, 2, half),
    ):
        for b in range(0, out_ref.shape[0], 2):
            partial = down_pair(hidden, downs, start + b, class_at(distance), depth)
            partial = partial.astype(jnp.bfloat16)
            out_ref[b] = partial[:, :depth]
            out_ref[b + 1] = partial[:, depth:]


def ffn(total, left, right, left2, right2, *weights):
    rows = left.shape[1]
    width, model = weights[-1].shape
    sent = jax.ShapeDtypeStruct(left.shape, jnp.bfloat16)
    half = jax.ShapeDtypeStruct(left2.shape, jnp.bfloat16)
    return pl.pallas_call(
        ffn_kernel,
        out_shape=(
            jax.ShapeDtypeStruct((rows, 2 * width), jnp.bfloat16),
            sent,
            sent,
            half,
            half,
        ),
        cost_estimate=cost(2 * rows * model * width * 4, 9000000),
        compiler_params=pltpu.CompilerParams(vmem_limit_bytes=20 << 20),
        name="ffn",
    )(total, left, right, left2, right2, *weights)


def own_down_kernel(hidden_ref, down_ref, down2_ref, out_ref):
    blocks, _, depth = out_ref.shape
    for b in range(0, blocks, 2):
        partial = down_pair(hidden_ref[...], (down_ref, down2_ref), b, class_at(0), depth)
        out_ref[b] = partial[:, :depth]
        out_ref[b + 1] = partial[:, depth:]


def own_down(hidden, down, down2):
    rows = hidden.shape[0]
    width, model = down.shape
    depth = model // (CLASSES * QUARTERS)
    return pl.pallas_call(
        own_down_kernel,
        out_shape=jax.ShapeDtypeStruct((QUARTERS, rows, depth), jnp.float32),
        cost_estimate=cost(rows * model * width, 4000000),
        compiler_params=pltpu.CompilerParams(vmem_limit_bytes=16 << 20),
        name="own_down",
    )(hidden, down, down2)


def join_kernel(own_ref, left_ref, right_ref, left2_ref, right2_ref, out_ref):
    blocks = own_ref.shape[0]
    chips = out_ref.shape[0]
    half = blocks // 2
    for q in range(blocks):
        both = own_ref[q] + left_ref[q].astype(jnp.float32) + right_ref[q].astype(jnp.float32)
        third = left2_ref[q] if q < half else right2_ref[q - half]
        both = (both + third.astype(jnp.float32)).astype(jnp.bfloat16)
        at = QUARTERS * MAIN + q * TAIL
        for chip in range(chips):
            tail = chips * MAIN + chip * TAIL
            out_ref[chip, q * MAIN : (q + 1) * MAIN] = both[chip * MAIN : (chip + 1) * MAIN]
            out_ref[chip, at : at + TAIL] = both[tail : tail + TAIL]


def join(own, left, right, left2, right2, chips):
    blocks, rows, depth = own.shape
    return pl.pallas_call(
        join_kernel,
        out_shape=jax.ShapeDtypeStruct((chips, blocks * CAP, depth), jnp.bfloat16),
        cost_estimate=cost(blocks * rows * depth, 12 * blocks * rows * depth),
        compiler_params=pltpu.CompilerParams(vmem_limit_bytes=16 << 20),
        name="join",
    )(own, left, right, left2, right2)


def combine_kernel(mix_ref, back_ref, out_ref):
    blocks, count, depth = out_ref.shape
    per_quarter = blocks // QUARTERS
    summed = lax.dot_general(
        mix_ref[...], back_ref[...], (((0,), (0,)), ((), ())), preferred_element_type=jnp.float32
    ).astype(jnp.bfloat16)
    for q in range(QUARTERS):
        for s in range(per_quarter):
            out_ref[q * per_quarter + s] = summed[
                q * count : (q + 1) * count, s * depth : (s + 1) * depth
            ]


def combine(mix, back, count, blocks):
    rows, quarter = back.shape
    depth = QUARTERS * quarter // blocks
    return pl.pallas_call(
        combine_kernel,
        out_shape=jax.ShapeDtypeStruct((blocks, count, depth), jnp.bfloat16),
        cost_estimate=cost(2 * rows * quarter * 128, 2400000),
        compiler_params=pltpu.CompilerParams(vmem_limit_bytes=12 << 20),
        name="combine",
    )(mix, back)


def on_device(tokens, expert_ids, route_logits, gate_weight, up_weight, down_weight):
    chips = lax.axis_size("x")
    parts = QUARTERS * CLASSES
    count, depth = tokens.shape
    swap = [(0, 1), (1, 0)]
    along = ("quarter", "class")
    ids = expert_ids.T

    def shift(value, distance):
        return lax.ppermute(value, along, [(i, (i + distance) % parts) for i in range(parts)])

    outgoing = dispatch(ids, lax.all_gather(tokens, "quarter"), chips)
    gate, up, down, outgoing = lax.optimization_barrier(
        (gate_weight, up_weight, down_weight, outgoing)
    )
    incoming = lax.all_to_all(outgoing, "x", 0, 0, tiled=True)
    gate2 = lax.ppermute(gate, "core", swap)
    up2 = lax.ppermute(up, "core", swap)
    down2 = lax.ppermute(down, "core", swap)
    own, low, high = unpack(incoming)
    left, right = shift(own, 1), shift(own, -1)
    left2, right2 = shift(low, 2), shift(high, -2)
    blocks = [w.reshape(QUARTERS, CLASSES, depth, w.shape[1]) for w in (gate, gate2, up, up2)]
    total = own_part(own, *blocks)
    hidden, to_right, to_left, to_right2, to_left2 = ffn(
        total, left, right, left2, right2, *blocks, down, down2
    )
    left, right = shift(to_right, 1), shift(to_left, -1)
    left2, right2 = shift(to_right2, 2), shift(to_left2, -2)
    partial_value = join(own_down(hidden, down, down2), left, right, left2, right2, chips)
    returned = lax.all_to_all(partial_value, "x", 0, 0, tiled=True)
    mix = mixing(ids, route_logits.T, chips)
    combined = combine(mix, returned.reshape(chips * QUARTERS * CAP, depth), count, QUARTERS)
    blocks = lax.all_to_all(combined, "quarter", 0, 0, tiled=True)
    return jnp.sum(blocks.astype(jnp.float32), axis=0).astype(jnp.bfloat16)


def solution(mesh):
    sizes = [mesh.shape[axis] for axis in ("rep", "exp", "tp")]
    devices = mesh.devices.reshape(sizes[0], sizes[1] // CORES, CORES, QUARTERS, CLASSES)
    split = Mesh(devices, ("rep", "x", "core", "quarter", "class"))
    tokens = ("rep", "x", "core")
    features = ("quarter", "class")
    hidden = ("x", "core", "quarter", "class")
    return jax.shard_map(
        on_device,
        mesh=split,
        in_specs=(
            P(tokens, features),
            P(tokens, None),
            P(tokens, None),
            P(None, hidden),
            P(None, hidden),
            P(hidden, None),
        ),
        out_specs=P(tokens, features),
        check_vma=False,
    )
```

```python
import functools

import jax
import jax.numpy as jnp
from jax import lax
from jax.experimental import pallas as pl
from jax.experimental.pallas import tpu as pltpu
from jax.sharding import Mesh, PartitionSpec as P


EXPERTS = 4
CAP = 20
MAIN = 16
TAIL = CAP - MAIN
QUARTERS = 4
CORES = 2


def cost(flops, nbytes):
    return pl.CostEstimate(flops=flops, bytes_accessed=nbytes, transcendentals=0)


def count_at_least(index, width, parts):
    total = jnp.zeros_like(index)
    for k in range(1, parts):
        total = total + (index >= k * width).astype(jnp.int32)
    return total


def placed(ids, expert, slot, before):
    chosen = ((ids[0:1, :] == expert) | (ids[1:2, :] == expert)).astype(jnp.float32)
    position = jnp.dot(chosen, before, preferred_element_type=jnp.float32)
    return chosen * (position == slot.astype(jnp.float32)).astype(jnp.float32)


def grouped(row, groups):
    later = row >= groups * MAIN
    rest = row - groups * MAIN
    main = count_at_least(row, MAIN, groups)
    tail = count_at_least(rest, TAIL, groups)
    group = jnp.where(later, tail, main)
    slot = jnp.where(later, MAIN + rest - TAIL * tail, row - MAIN * main)
    return group, slot


def dispatch_kernel(chips, ids_ref, tokens_ref, out_ref):
    count = tokens_ref.shape[0]
    row = lax.broadcasted_iota(jnp.int32, (EXPERTS * CAP, count), 0)
    expert = count_at_least(row, CAP, EXPERTS)
    slot = row - CAP * expert
    first = lax.broadcasted_iota(jnp.int32, (count, count), 0)
    second = lax.broadcasted_iota(jnp.int32, (count, count), 1)
    before = (first < second).astype(jnp.float32)
    placement = placed(ids_ref[...], expert, slot, before).astype(jnp.bfloat16)
    slots = jnp.dot(placement, tokens_ref[...], preferred_element_type=jnp.float32).astype(
        jnp.bfloat16
    )
    per_expert = chips // EXPERTS
    for chip in range(chips):
        e = chip // per_expert
        out_ref[chip] = slots[e * CAP : (e + 1) * CAP]


def dispatch(ids, tokens, chips):
    count, features = tokens.shape
    return pl.pallas_call(
        functools.partial(dispatch_kernel, chips),
        out_shape=jax.ShapeDtypeStruct((chips, CAP, features), jnp.bfloat16),
        cost_estimate=cost(2 * EXPERTS * CAP * count * features, 200000),
        compiler_params=pltpu.CompilerParams(vmem_limit_bytes=60 << 20),
        name="dispatch",
    )(ids, tokens)


def gather_rows_kernel(in_ref, out_ref):
    chips = in_ref.shape[0]
    for chip in range(chips):
        out_ref[chip * MAIN : (chip + 1) * MAIN] = in_ref[chip, :MAIN]
        at = chips * MAIN + chip * TAIL
        out_ref[at : at + TAIL] = in_ref[chip, MAIN:]


def gather_rows(slots):
    chips, _, depth = slots.shape
    return pl.pallas_call(
        gather_rows_kernel,
        out_shape=jax.ShapeDtypeStruct((chips * CAP, depth), jnp.bfloat16),
        cost_estimate=cost(1000, 250000),
        compiler_params=pltpu.CompilerParams(vmem_limit_bytes=4 << 20),
        name="gather_rows",
    )(slots)


def mixing_kernel(chips, count, ids_ref, logits_ref, out_ref):
    lanes = ids_ref.shape[1]
    rows = chips * QUARTERS * CAP
    row = lax.broadcasted_iota(jnp.int32, (rows, lanes), 0)
    chip = count_at_least(row, QUARTERS * CAP, chips)
    quarter, slot = grouped(row - QUARTERS * CAP * chip, QUARTERS)
    expert = count_at_least(chip, chips // EXPERTS, EXPERTS)
    lane = lax.broadcasted_iota(jnp.int32, (rows, lanes), 1)
    own = (count_at_least(lane, count, QUARTERS) == quarter).astype(jnp.float32)
    first = lax.broadcasted_iota(jnp.int32, (lanes, lanes), 0)
    second = lax.broadcasted_iota(jnp.int32, (lanes, lanes), 1)
    same = count_at_least(first, count, QUARTERS) == count_at_least(second, count, QUARTERS)
    before = ((first < second) & same).astype(jnp.float32)
    ids = ids_ref[...]
    diff = logits_ref[0:1, :] - logits_ref[1:2, :]
    share = jnp.where(ids[0:1, :] == expert, jax.nn.sigmoid(diff), jax.nn.sigmoid(-diff))
    out_ref[...] = (placed(ids, expert, slot, before) * share * own).astype(jnp.bfloat16)


def mixing(ids, logits, chips):
    count = ids.shape[1]
    rows = chips * QUARTERS * CAP
    return pl.pallas_call(
        functools.partial(mixing_kernel, chips, count),
        out_shape=jax.ShapeDtypeStruct((rows, QUARTERS * count), jnp.bfloat16),
        cost_estimate=cost(2 * rows * 128 * 128, 200000),
        compiler_params=pltpu.CompilerParams(vmem_limit_bytes=8 << 20),
        name="mixing",
    )(jnp.tile(ids, (1, QUARTERS)), jnp.tile(logits, (1, QUARTERS)))


def side_by_side(refs, b, parity):
    return jnp.concatenate([ref[b, parity] for ref in refs], axis=1)


def multiply(total, tokens, refs, parity, start):
    for b in range(0, tokens.shape[0], 2):
        rows = jnp.concatenate([tokens[b], tokens[b + 1]], axis=1)
        weight = jnp.concatenate(
            [side_by_side(refs, start + b, parity), side_by_side(refs, start + b + 1, parity)],
            axis=0,
        )
        added = jnp.dot(rows, weight, preferred_element_type=jnp.float32)
        total = added if total is None else total + added
    return total


def own_kernel(slots_ref, gate_ref, gate2_ref, up_ref, up2_ref, out_ref):
    refs = (gate_ref, gate2_ref, up_ref, up2_ref)
    out_ref[...] = multiply(None, slots_ref, refs, lax.axis_index("odd"), 0)


def own_part(slots, *weights):
    pairs, rows, depth = slots.shape
    width = weights[0].shape[-1]
    return pl.pallas_call(
        own_kernel,
        out_shape=jax.ShapeDtypeStruct((rows, 4 * width), jnp.float32),
        cost_estimate=cost(2 * pairs * rows * depth * 4 * width, 4200000),
        compiler_params=pltpu.CompilerParams(vmem_limit_bytes=16 << 20),
        name="own_part",
    )(slots, *weights)


def down_pair(hidden, refs, b, parity, depth):
    def block(b):
        lanes = pl.ds(pl.multiple_of((2 * b + parity) * depth, 128), depth)
        return jnp.concatenate([ref[:, lanes] for ref in refs], axis=0)

    weight = jnp.concatenate([block(b), block(b + 1)], axis=1)
    return jnp.dot(hidden, weight, preferred_element_type=jnp.float32)


def ffn_kernel(
    total_ref, early_ref, late_ref, gate_ref, gate2_ref, up_ref, up2_ref, down_ref, down2_ref, hidden_ref, send_early_ref, send_late_ref
):
    half, _, depth = early_ref.shape
    parity = 1 - lax.axis_index("odd")
    early = half * (1 - lax.axis_index("core"))
    late = half - early
    width = gate_ref.shape[-1]
    refs = (gate_ref, gate2_ref, up_ref, up2_ref)
    total = multiply(total_ref[...], early_ref, refs, parity, early)
    total = multiply(total, late_ref, refs, parity, late)
    gate = total[:, : 2 * width]
    hidden = (gate * jax.nn.sigmoid(gate) * total[:, 2 * width :]).astype(jnp.bfloat16)
    hidden_ref[...] = hidden
    for out_ref, start in ((send_early_ref, early), (send_late_ref, late)):
        for b in range(0, half, 2):
            partial = down_pair(hidden, (down_ref, down2_ref), start + b, parity, depth)
            partial = partial.astype(jnp.bfloat16)
            out_ref[b] = partial[:, :depth]
            out_ref[b + 1] = partial[:, depth:]


def ffn(total, early, late, *weights):
    _, rows, _ = early.shape
    width, model = weights[-1].shape
    sent = jax.ShapeDtypeStruct(early.shape, jnp.bfloat16)
    return pl.pallas_call(
        ffn_kernel,
        out_shape=(jax.ShapeDtypeStruct((rows, 2 * width), jnp.bfloat16), sent, sent),
        cost_estimate=cost(2 * rows * model * width * 3, 7000000),
        compiler_params=pltpu.CompilerParams(vmem_limit_bytes=20 << 20),
        name="ffn",
    )(total, early, late, *weights)


def own_down_kernel(hidden_ref, down_ref, down2_ref, out_ref):
    pairs, _, depth = out_ref.shape
    parity = lax.axis_index("odd")
    for b in range(0, pairs, 2):
        partial = down_pair(hidden_ref[...], (down_ref, down2_ref), b, parity, depth)
        out_ref[b] = partial[:, :depth]
        out_ref[b + 1] = partial[:, depth:]


def own_down(hidden, down, down2, pairs):
    rows = hidden.shape[0]
    width, model = down.shape
    depth = model // (2 * pairs)
    return pl.pallas_call(
        own_down_kernel,
        out_shape=jax.ShapeDtypeStruct((pairs, rows, depth), jnp.float32),
        cost_estimate=cost(2 * rows * model * width, 4000000),
        compiler_params=pltpu.CompilerParams(vmem_limit_bytes=16 << 20),
        name="own_down",
    )(hidden, down, down2)


def join_kernel(own_ref, early_ref, late_ref, out_ref):
    pairs, _, depth = own_ref.shape
    chips = out_ref.shape[0]
    half = pairs // 2
    upward = lax.axis_index("core") == 1
    per_quarter = pairs // QUARTERS
    for b in range(pairs):
        lower = b < half
        i = b if lower else b - half
        other = jnp.where(upward == lower, early_ref[i], late_ref[i])
        both = (own_ref[b] + other.astype(jnp.float32)).astype(jnp.bfloat16)
        q, s = b // per_quarter, b % per_quarter
        at = QUARTERS * MAIN + q * TAIL
        lanes = slice(s * depth, (s + 1) * depth)
        for chip in range(chips):
            tail = chips * MAIN + chip * TAIL
            out_ref[chip, q * MAIN : (q + 1) * MAIN, lanes] = both[chip * MAIN : (chip + 1) * MAIN]
            out_ref[chip, at : at + TAIL, lanes] = both[tail : tail + TAIL]


def join(own, early, late, chips):
    pairs, rows, depth = own.shape
    out = (chips, QUARTERS * CAP, pairs * depth // QUARTERS)
    return pl.pallas_call(
        join_kernel,
        out_shape=jax.ShapeDtypeStruct(out, jnp.bfloat16),
        cost_estimate=cost(pairs * rows * depth, 8 * pairs * rows * depth),
        compiler_params=pltpu.CompilerParams(vmem_limit_bytes=16 << 20),
        name="join",
    )(own, early, late)


def combine_kernel(mix_ref, back_ref, out_ref):
    blocks, count, depth = out_ref.shape
    per_quarter = blocks // QUARTERS
    summed = lax.dot_general(
        mix_ref[...], back_ref[...], (((0,), (0,)), ((), ())), preferred_element_type=jnp.float32
    ).astype(jnp.bfloat16)
    for q in range(QUARTERS):
        for s in range(per_quarter):
            out_ref[q * per_quarter + s] = summed[
                q * count : (q + 1) * count, s * depth : (s + 1) * depth
            ]


def combine(mix, back, count, blocks):
    rows, quarter = back.shape
    depth = QUARTERS * quarter // blocks
    return pl.pallas_call(
        combine_kernel,
        out_shape=jax.ShapeDtypeStruct((blocks, count, depth), jnp.bfloat16),
        cost_estimate=cost(2 * rows * quarter * 128, 2400000),
        compiler_params=pltpu.CompilerParams(vmem_limit_bytes=12 << 20),
        name="combine",
    )(mix, back)


def on_device(tokens, expert_ids, route_logits, gate_weight, up_weight, down_weight):
    chips = lax.axis_size("x")
    pairs = lax.axis_size("pair")
    parts = 2 * pairs
    count, depth = tokens.shape
    swap = [(0, 1), (1, 0)]
    ids = expert_ids.T
    along = ("core", "pair", "odd")
    half = pairs // 2

    def exchange(early, late):
        def shift(value, core_up):
            steps = [(c, 1 if c == core_up else -1) for c in range(CORES)]
            return lax.ppermute(
                value,
                along,
                [(c * parts + z, c * parts + (z + to) % parts) for c, to in steps for z in range(parts)],
            )

        return shift(early, 1), shift(late, 0)

    outgoing = dispatch(ids, tokens, chips)
    gate, up, down, outgoing = lax.optimization_barrier(
        (gate_weight, up_weight, down_weight, outgoing)
    )
    incoming = lax.all_to_all(outgoing, "x", 0, 0, tiled=True)
    gate2 = lax.ppermute(gate, "core", swap)
    up2 = lax.ppermute(up, "core", swap)
    down2 = lax.ppermute(down, "core", swap)
    own = lax.all_gather(gather_rows(incoming), "pair")
    first = half * (1 - lax.axis_index("core"))
    early, late = exchange(
        lax.dynamic_slice_in_dim(own, first, half), lax.dynamic_slice_in_dim(own, half - first, half)
    )
    blocks = [w.reshape(pairs, 2, depth, w.shape[1]) for w in (gate, gate2, up, up2)]
    total = own_part(own, *blocks)
    hidden, early, late = ffn(total, early, late, *blocks, down, down2)
    early, late = exchange(early, late)
    partial_value = join(own_down(hidden, down, down2, pairs), early, late, chips)
    returned = lax.all_to_all(partial_value, "x", 0, 0, tiled=True)
    mix = mixing(ids, route_logits.T, chips)
    back = returned.reshape(chips * QUARTERS * CAP, pairs * depth // QUARTERS)
    combined = combine(mix, back, count, pairs)
    blocks = lax.all_to_all(combined, "pair", 0, 0, tiled=True)
    return jnp.sum(blocks.astype(jnp.float32), axis=0).astype(jnp.bfloat16)


def solution(mesh):
    sizes = [mesh.shape[axis] for axis in ("rep", "exp", "tp")]
    devices = mesh.devices.reshape(sizes[0], sizes[1] // CORES, CORES, sizes[2] // 2, 2)
    split = Mesh(devices, ("rep", "x", "core", "pair", "odd"))
    tokens = ("rep", "x", "core")
    features = ("pair", "odd")
    hidden = ("x", "core", "pair", "odd")
    return jax.shard_map(
        on_device,
        mesh=split,
        in_specs=(
            P(tokens, features),
            P(tokens, None),
            P(tokens, None),
            P(None, hidden),
            P(None, hidden),
            P(hidden, None),
        ),
        out_specs=P(tokens, features),
        check_vma=False,
    )
```

```python
import functools

import jax
import jax.numpy as jnp
from jax import lax
from jax.experimental import pallas as pl
from jax.experimental.pallas import tpu as pltpu
from jax.sharding import Mesh, PartitionSpec as P


EXPERTS = 4
CAP = 20
MAIN = 16
TAIL = CAP - MAIN
QUARTERS = 4
CORES = 2


def cost(flops, nbytes):
    return pl.CostEstimate(flops=flops, bytes_accessed=nbytes, transcendentals=0)


def count_at_least(index, width, parts):
    total = jnp.zeros_like(index)
    for k in range(1, parts):
        total = total + (index >= k * width).astype(jnp.int32)
    return total


def placed(ids, expert, slot, before):
    chosen = ((ids[0:1, :] == expert) | (ids[1:2, :] == expert)).astype(jnp.float32)
    position = jnp.dot(chosen, before, preferred_element_type=jnp.float32)
    return chosen * (position == slot.astype(jnp.float32)).astype(jnp.float32)


def grouped(row, groups):
    later = row >= groups * MAIN
    rest = row - groups * MAIN
    main = count_at_least(row, MAIN, groups)
    tail = count_at_least(rest, TAIL, groups)
    group = jnp.where(later, tail, main)
    slot = jnp.where(later, MAIN + rest - TAIL * tail, row - MAIN * main)
    return group, slot


def dispatch_kernel(chips, ids_ref, tokens_ref, out_ref):
    count = tokens_ref.shape[0]
    row = lax.broadcasted_iota(jnp.int32, (EXPERTS * CAP, count), 0)
    expert = count_at_least(row, CAP, EXPERTS)
    slot = row - CAP * expert
    first = lax.broadcasted_iota(jnp.int32, (count, count), 0)
    second = lax.broadcasted_iota(jnp.int32, (count, count), 1)
    before = (first < second).astype(jnp.float32)
    placement = placed(ids_ref[...], expert, slot, before).astype(jnp.bfloat16)
    slots = jnp.dot(placement, tokens_ref[...], preferred_element_type=jnp.float32).astype(
        jnp.bfloat16
    )
    per_expert = chips // EXPERTS
    for chip in range(chips):
        e = chip // per_expert
        out_ref[chip] = slots[e * CAP : (e + 1) * CAP]


def dispatch(ids, tokens, chips):
    count, features = tokens.shape
    return pl.pallas_call(
        functools.partial(dispatch_kernel, chips),
        out_shape=jax.ShapeDtypeStruct((chips, CAP, features), jnp.bfloat16),
        cost_estimate=cost(2 * EXPERTS * CAP * count * features, 200000),
        compiler_params=pltpu.CompilerParams(vmem_limit_bytes=60 << 20),
        name="dispatch",
    )(ids, tokens)


def gather_rows_kernel(in_ref, out_ref):
    chips = in_ref.shape[0]
    for chip in range(chips):
        out_ref[chip * MAIN : (chip + 1) * MAIN] = in_ref[chip, :MAIN]
        at = chips * MAIN + chip * TAIL
        out_ref[at : at + TAIL] = in_ref[chip, MAIN:]


def gather_rows(slots):
    chips, _, depth = slots.shape
    return pl.pallas_call(
        gather_rows_kernel,
        out_shape=jax.ShapeDtypeStruct((chips * CAP, depth), jnp.bfloat16),
        cost_estimate=cost(1000, 250000),
        compiler_params=pltpu.CompilerParams(vmem_limit_bytes=4 << 20),
        name="gather_rows",
    )(slots)


def mixing_kernel(chips, count, ids_ref, logits_ref, out_ref):
    lanes = ids_ref.shape[1]
    rows = chips * QUARTERS * CAP
    row = lax.broadcasted_iota(jnp.int32, (rows, lanes), 0)
    chip = count_at_least(row, QUARTERS * CAP, chips)
    quarter, slot = grouped(row - QUARTERS * CAP * chip, QUARTERS)
    expert = count_at_least(chip, chips // EXPERTS, EXPERTS)
    lane = lax.broadcasted_iota(jnp.int32, (rows, lanes), 1)
    own = (count_at_least(lane, count, QUARTERS) == quarter).astype(jnp.float32)
    first = lax.broadcasted_iota(jnp.int32, (lanes, lanes), 0)
    second = lax.broadcasted_iota(jnp.int32, (lanes, lanes), 1)
    same = count_at_least(first, count, QUARTERS) == count_at_least(second, count, QUARTERS)
    before = ((first < second) & same).astype(jnp.float32)
    ids = ids_ref[...]
    diff = logits_ref[0:1, :] - logits_ref[1:2, :]
    share = jnp.where(ids[0:1, :] == expert, jax.nn.sigmoid(diff), jax.nn.sigmoid(-diff))
    out_ref[...] = (placed(ids, expert, slot, before) * share * own).astype(jnp.bfloat16)


def mixing(ids, logits, chips):
    count = ids.shape[1]
    rows = chips * QUARTERS * CAP
    return pl.pallas_call(
        functools.partial(mixing_kernel, chips, count),
        out_shape=jax.ShapeDtypeStruct((rows, QUARTERS * count), jnp.bfloat16),
        cost_estimate=cost(2 * rows * 128 * 128, 200000),
        compiler_params=pltpu.CompilerParams(vmem_limit_bytes=8 << 20),
        name="mixing",
    )(jnp.tile(ids, (1, QUARTERS)), jnp.tile(logits, (1, QUARTERS)))


def side_by_side(refs, b, parity):
    return jnp.concatenate([ref[b, parity] for ref in refs], axis=1)


def multiply(total, tokens, refs, parity, start):
    for b in range(0, tokens.shape[0], 2):
        rows = jnp.concatenate([tokens[b], tokens[b + 1]], axis=1)
        weight = jnp.concatenate(
            [side_by_side(refs, start + b, parity), side_by_side(refs, start + b + 1, parity)],
            axis=0,
        )
        added = jnp.dot(rows, weight, preferred_element_type=jnp.float32)
        total = added if total is None else total + added
    return total


def own_kernel(slots_ref, gate_ref, gate2_ref, up_ref, up2_ref, out_ref):
    refs = (gate_ref, gate2_ref, up_ref, up2_ref)
    out_ref[...] = multiply(None, slots_ref, refs, lax.axis_index("odd"), 0)


def own_part(slots, *weights):
    pairs, rows, depth = slots.shape
    width = weights[0].shape[-1]
    return pl.pallas_call(
        own_kernel,
        out_shape=jax.ShapeDtypeStruct((rows, 4 * width), jnp.float32),
        cost_estimate=cost(2 * pairs * rows * depth * 4 * width, 4200000),
        compiler_params=pltpu.CompilerParams(vmem_limit_bytes=16 << 20),
        name="own_part",
    )(slots, *weights)


def down_pair(hidden, refs, b, parity, depth):
    def block(b):
        lanes = pl.ds(pl.multiple_of((2 * b + parity) * depth, 128), depth)
        return jnp.concatenate([ref[:, lanes] for ref in refs], axis=0)

    weight = jnp.concatenate([block(b), block(b + 1)], axis=1)
    return jnp.dot(hidden, weight, preferred_element_type=jnp.float32)


def ffn_kernel(
    total_ref, inside_ref, outside_ref, gate_ref, gate2_ref, up_ref, up2_ref, down_ref, down2_ref, hidden_ref, to_inside_ref, to_outside_ref
):
    half, _, depth = inside_ref.shape
    parity = 1 - lax.axis_index("odd")
    width = gate_ref.shape[-1]
    refs = (gate_ref, gate2_ref, up_ref, up2_ref)
    total = multiply(total_ref[...], inside_ref, refs, parity, 0)
    total = multiply(total, outside_ref, refs, parity, half)
    gate = total[:, : 2 * width]
    hidden = (gate * jax.nn.sigmoid(gate) * total[:, 2 * width :]).astype(jnp.bfloat16)
    hidden_ref[...] = hidden
    for b in range(0, 2 * half, 2):
        partial = down_pair(hidden, (down_ref, down2_ref), b, parity, depth).astype(jnp.bfloat16)
        out_ref, at = (to_inside_ref, b) if b < half else (to_outside_ref, b - half)
        out_ref[at] = partial[:, :depth]
        out_ref[at + 1] = partial[:, depth:]


def ffn(total, inside, outside, *weights):
    _, rows, _ = inside.shape
    width, model = weights[-1].shape
    sent = jax.ShapeDtypeStruct(inside.shape, jnp.bfloat16)
    return pl.pallas_call(
        ffn_kernel,
        out_shape=(jax.ShapeDtypeStruct((rows, 2 * width), jnp.bfloat16), sent, sent),
        cost_estimate=cost(2 * rows * model * width * 3, 7000000),
        compiler_params=pltpu.CompilerParams(vmem_limit_bytes=20 << 20),
        name="ffn",
    )(total, inside, outside, *weights)


def own_down_kernel(hidden_ref, down_ref, down2_ref, out_ref):
    pairs, _, depth = out_ref.shape
    parity = lax.axis_index("odd")
    for b in range(0, pairs, 2):
        partial = down_pair(hidden_ref[...], (down_ref, down2_ref), b, parity, depth)
        out_ref[b] = partial[:, :depth]
        out_ref[b + 1] = partial[:, depth:]


def own_down(hidden, down, down2, pairs):
    rows = hidden.shape[0]
    width, model = down.shape
    depth = model // (2 * pairs)
    return pl.pallas_call(
        own_down_kernel,
        out_shape=jax.ShapeDtypeStruct((pairs, rows, depth), jnp.float32),
        cost_estimate=cost(2 * rows * model * width, 4000000),
        compiler_params=pltpu.CompilerParams(vmem_limit_bytes=16 << 20),
        name="own_down",
    )(hidden, down, down2)


def join_kernel(own_ref, inside_ref, outside_ref, out_ref):
    pairs, _, depth = own_ref.shape
    chips = out_ref.shape[0]
    half = pairs // 2
    per_quarter = pairs // QUARTERS
    for b in range(pairs):
        other = inside_ref[b] if b < half else outside_ref[b - half]
        both = (own_ref[b] + other.astype(jnp.float32)).astype(jnp.bfloat16)
        q, s = b // per_quarter, b % per_quarter
        at = QUARTERS * MAIN + q * TAIL
        lanes = slice(s * depth, (s + 1) * depth)
        for chip in range(chips):
            tail = chips * MAIN + chip * TAIL
            out_ref[chip, q * MAIN : (q + 1) * MAIN, lanes] = both[chip * MAIN : (chip + 1) * MAIN]
            out_ref[chip, at : at + TAIL, lanes] = both[tail : tail + TAIL]


def join(own, inside, outside, chips):
    pairs, rows, depth = own.shape
    out = (chips, QUARTERS * CAP, pairs * depth // QUARTERS)
    return pl.pallas_call(
        join_kernel,
        out_shape=jax.ShapeDtypeStruct(out, jnp.bfloat16),
        cost_estimate=cost(pairs * rows * depth, 8 * pairs * rows * depth),
        compiler_params=pltpu.CompilerParams(vmem_limit_bytes=16 << 20),
        name="join",
    )(own, inside, outside)


def combine_kernel(mix_ref, back_ref, out_ref):
    blocks, count, depth = out_ref.shape
    per_quarter = blocks // QUARTERS
    summed = lax.dot_general(
        mix_ref[...], back_ref[...], (((0,), (0,)), ((), ())), preferred_element_type=jnp.float32
    ).astype(jnp.bfloat16)
    for q in range(QUARTERS):
        for s in range(per_quarter):
            out_ref[q * per_quarter + s] = summed[
                q * count : (q + 1) * count, s * depth : (s + 1) * depth
            ]


def combine(mix, back, count, blocks):
    rows, quarter = back.shape
    depth = QUARTERS * quarter // blocks
    return pl.pallas_call(
        combine_kernel,
        out_shape=jax.ShapeDtypeStruct((blocks, count, depth), jnp.bfloat16),
        cost_estimate=cost(2 * rows * quarter * 128, 2400000),
        compiler_params=pltpu.CompilerParams(vmem_limit_bytes=12 << 20),
        name="combine",
    )(mix, back)


def on_device(tokens, expert_ids, route_logits, gate_weight, up_weight, down_weight):
    chips = lax.axis_size("x")
    pairs = lax.axis_size("pair")
    parts = 2 * pairs
    count, depth = tokens.shape
    swap = [(0, 1), (1, 0)]
    along = ("pair", "odd")
    ids = expert_ids.T
    inner = [(z, z + 1 if z % 2 == 0 else z - 1) for z in range(parts)]
    outer = [(z, (z - 1 if z % 2 == 0 else z + 1) % parts) for z in range(parts)]
    outgoing = dispatch(ids, tokens, chips)
    gate, up, down, outgoing = lax.optimization_barrier(
        (gate_weight, up_weight, down_weight, outgoing)
    )
    incoming = lax.all_to_all(outgoing, "x", 0, 0, tiled=True)
    gate2 = lax.ppermute(gate, "core", swap)
    up2 = lax.ppermute(up, "core", swap)
    down2 = lax.ppermute(down, "core", swap)
    own = lax.all_gather(gather_rows(incoming), "pair")
    inside = lax.ppermute(own[: pairs // 2], along, inner)
    outside = lax.ppermute(own[pairs // 2 :], along, outer)
    blocks = [w.reshape(pairs, 2, depth, w.shape[1]) for w in (gate, gate2, up, up2)]
    total = own_part(own, *blocks)
    hidden, inside, outside = ffn(total, inside, outside, *blocks, down, down2)
    inside = lax.ppermute(inside, along, inner)
    outside = lax.ppermute(outside, along, outer)
    partial_value = join(own_down(hidden, down, down2, pairs), inside, outside, chips)
    returned = lax.all_to_all(partial_value, "x", 0, 0, tiled=True)
    mix = mixing(ids, route_logits.T, chips)
    back = returned.reshape(chips * QUARTERS * CAP, pairs * depth // QUARTERS)
    combined = combine(mix, back, count, pairs)
    blocks = lax.all_to_all(combined, "pair", 0, 0, tiled=True)
    return jnp.sum(blocks.astype(jnp.float32), axis=0).astype(jnp.bfloat16)


def solution(mesh):
    sizes = [mesh.shape[axis] for axis in ("rep", "exp", "tp")]
    devices = mesh.devices.reshape(sizes[0], sizes[1] // CORES, CORES, sizes[2] // 2, 2)
    split = Mesh(devices, ("rep", "x", "core", "pair", "odd"))
    tokens = ("rep", "x", "core")
    features = ("pair", "odd")
    hidden = ("x", "core", "pair", "odd")
    return jax.shard_map(
        on_device,
        mesh=split,
        in_specs=(
            P(tokens, features),
            P(tokens, None),
            P(tokens, None),
            P(None, hidden),
            P(None, hidden),
            P(hidden, None),
        ),
        out_specs=P(tokens, features),
        check_vma=False,
    )
```

```python
import functools

import jax
import jax.numpy as jnp
from jax import lax
from jax.experimental import pallas as pl
from jax.experimental.pallas import tpu as pltpu
from jax.sharding import Mesh, PartitionSpec as P


EXPERTS = 4
CAP = 20
MAIN = 16
TAIL = CAP - MAIN
QUARTERS = 4
CLASSES = 4
CORES = 2


def cost(flops, nbytes):
    return pl.CostEstimate(flops=flops, bytes_accessed=nbytes, transcendentals=0)


def count_at_least(index, width, parts):
    total = jnp.zeros_like(index)
    for k in range(1, parts):
        total = total + (index >= k * width).astype(jnp.int32)
    return total


def placed(ids, expert, slot, before):
    chosen = ((ids[0:1, :] == expert) | (ids[1:2, :] == expert)).astype(jnp.float32)
    position = jnp.dot(chosen, before, preferred_element_type=jnp.float32)
    return chosen * (position == slot.astype(jnp.float32)).astype(jnp.float32)


def grouped(row, groups):
    later = row >= groups * MAIN
    rest = row - groups * MAIN
    main = count_at_least(row, MAIN, groups)
    tail = count_at_least(rest, TAIL, groups)
    group = jnp.where(later, tail, main)
    slot = jnp.where(later, MAIN + rest - TAIL * tail, row - MAIN * main)
    return group, slot


def dispatch_kernel(chips, ids_ref, tokens_ref, out_ref):
    count = tokens_ref.shape[0]
    row = lax.broadcasted_iota(jnp.int32, (EXPERTS * CAP, count), 0)
    expert = count_at_least(row, CAP, EXPERTS)
    slot = row - CAP * expert
    first = lax.broadcasted_iota(jnp.int32, (count, count), 0)
    second = lax.broadcasted_iota(jnp.int32, (count, count), 1)
    before = (first < second).astype(jnp.float32)
    placement = placed(ids_ref[...], expert, slot, before).astype(jnp.bfloat16)
    slots = jnp.dot(placement, tokens_ref[...], preferred_element_type=jnp.float32).astype(
        jnp.bfloat16
    )
    per_expert = chips // EXPERTS
    for chip in range(chips):
        e = chip // per_expert
        out_ref[chip] = slots[e * CAP : (e + 1) * CAP]


def dispatch(ids, tokens, chips):
    count, features = tokens.shape
    return pl.pallas_call(
        functools.partial(dispatch_kernel, chips),
        out_shape=jax.ShapeDtypeStruct((chips, CAP, features), jnp.bfloat16),
        cost_estimate=cost(2 * EXPERTS * CAP * count * features, 200000),
        compiler_params=pltpu.CompilerParams(vmem_limit_bytes=60 << 20),
        name="dispatch",
    )(ids, tokens)


def gather_rows_kernel(in_ref, out_ref):
    chips = in_ref.shape[0]
    for chip in range(chips):
        out_ref[chip * MAIN : (chip + 1) * MAIN] = in_ref[chip, :MAIN]
        at = chips * MAIN + chip * TAIL
        out_ref[at : at + TAIL] = in_ref[chip, MAIN:]


def gather_rows(slots):
    chips, _, depth = slots.shape
    return pl.pallas_call(
        gather_rows_kernel,
        out_shape=jax.ShapeDtypeStruct((chips * CAP, depth), jnp.bfloat16),
        cost_estimate=cost(1000, 250000),
        compiler_params=pltpu.CompilerParams(vmem_limit_bytes=4 << 20),
        name="gather_rows",
    )(slots)


def mixing_kernel(chips, count, ids_ref, logits_ref, out_ref):
    lanes = ids_ref.shape[1]
    rows = chips * QUARTERS * CAP
    row = lax.broadcasted_iota(jnp.int32, (rows, lanes), 0)
    chip = count_at_least(row, QUARTERS * CAP, chips)
    quarter, slot = grouped(row - QUARTERS * CAP * chip, QUARTERS)
    expert = count_at_least(chip, chips // EXPERTS, EXPERTS)
    lane = lax.broadcasted_iota(jnp.int32, (rows, lanes), 1)
    own = (count_at_least(lane, count, QUARTERS) == quarter).astype(jnp.float32)
    first = lax.broadcasted_iota(jnp.int32, (lanes, lanes), 0)
    second = lax.broadcasted_iota(jnp.int32, (lanes, lanes), 1)
    same = count_at_least(first, count, QUARTERS) == count_at_least(second, count, QUARTERS)
    before = ((first < second) & same).astype(jnp.float32)
    ids = ids_ref[...]
    diff = logits_ref[0:1, :] - logits_ref[1:2, :]
    share = jnp.where(ids[0:1, :] == expert, jax.nn.sigmoid(diff), jax.nn.sigmoid(-diff))
    out_ref[...] = (placed(ids, expert, slot, before) * share * own).astype(jnp.bfloat16)


def mixing(ids, logits, chips):
    count = ids.shape[1]
    rows = chips * QUARTERS * CAP
    return pl.pallas_call(
        functools.partial(mixing_kernel, chips, count),
        out_shape=jax.ShapeDtypeStruct((rows, QUARTERS * count), jnp.bfloat16),
        cost_estimate=cost(2 * rows * 128 * 128, 200000),
        compiler_params=pltpu.CompilerParams(vmem_limit_bytes=8 << 20),
        name="mixing",
    )(jnp.tile(ids, (1, QUARTERS)), jnp.tile(logits, (1, QUARTERS)))


def class_at(distance):
    own = 2 * lax.axis_index("half") + lax.axis_index("odd")
    return lax.rem(own + CLASSES + distance, CLASSES)


def side_by_side(refs, b, parity):
    return jnp.concatenate([ref[b, parity] for ref in refs], axis=1)


def multiply(total, tokens, refs, parity, start):
    for b in range(0, tokens.shape[0], 2):
        rows = jnp.concatenate([tokens[b], tokens[b + 1]], axis=1)
        weight = jnp.concatenate(
            [side_by_side(refs, start + b, parity), side_by_side(refs, start + b + 1, parity)],
            axis=0,
        )
        added = jnp.dot(rows, weight, preferred_element_type=jnp.float32)
        total = added if total is None else total + added
    return total


def own_kernel(slots_ref, gate_ref, gate2_ref, up_ref, up2_ref, out_ref):
    refs = (gate_ref, gate2_ref, up_ref, up2_ref)
    out_ref[...] = multiply(None, slots_ref, refs, lax.axis_index("odd"), 0)


def own_part(slots, *weights):
    pairs, rows, depth = slots.shape
    width = weights[0].shape[-1]
    return pl.pallas_call(
        own_kernel,
        out_shape=jax.ShapeDtypeStruct((rows, 4 * width), jnp.float32),
        cost_estimate=cost(2 * pairs * rows * depth * 4 * width, 4200000),
        compiler_params=pltpu.CompilerParams(vmem_limit_bytes=16 << 20),
        name="own_part",
    )(slots, *weights)


def down_pair(hidden, refs, q, kind, depth):
    def block(q):
        lanes = pl.ds(pl.multiple_of((CLASSES * q + kind) * depth, 128), depth)
        return jnp.concatenate([ref[:, lanes] for ref in refs], axis=0)

    weight = jnp.concatenate([block(q), block(q + 1)], axis=1)
    return jnp.dot(hidden, weight, preferred_element_type=jnp.float32)


def ffn_kernel(
    total_ref, left_ref, right_ref, gate_ref, gate2_ref, up_ref, up2_ref, down_ref, down2_ref, hidden_ref, to_right_ref, to_left_ref, to_right2_ref, to_left2_ref
):
    pairs, _, depth = left_ref.shape
    parity = 1 - lax.axis_index("odd")
    width = gate_ref.shape[-1]
    half = QUARTERS // 2
    refs = (gate_ref, gate2_ref, up_ref, up2_ref)
    total = multiply(total_ref[...], left_ref, refs, parity, 0)
    total = multiply(total, right_ref, refs, parity, pairs)
    gate = total[:, : 2 * width]
    hidden = (gate * jax.nn.sigmoid(gate) * total[:, 2 * width :]).astype(jnp.bfloat16)
    hidden_ref[...] = hidden
    downs = (down_ref, down2_ref)
    for out_ref, distance, start in (
        (to_right_ref, 1, 0),
        (to_left_ref, -1, 0),
        (to_right2_ref, 2, 0),
        (to_left2_ref, 2, half),
    ):
        for b in range(0, out_ref.shape[0], 2):
            partial = down_pair(hidden, downs, start + b, class_at(distance), depth)
            partial = partial.astype(jnp.bfloat16)
            out_ref[b] = partial[:, :depth]
            out_ref[b + 1] = partial[:, depth:]


def ffn(total, left, right, *weights):
    rows, depth = left.shape[1:]
    width, model = weights[-1].shape
    sent = jax.ShapeDtypeStruct((QUARTERS, rows, depth), jnp.bfloat16)
    half = jax.ShapeDtypeStruct((QUARTERS // 2, rows, depth), jnp.bfloat16)
    return pl.pallas_call(
        ffn_kernel,
        out_shape=(
            jax.ShapeDtypeStruct((rows, 2 * width), jnp.bfloat16),
            sent,
            sent,
            half,
            half,
        ),
        cost_estimate=cost(2 * rows * model * width * 4, 9000000),
        compiler_params=pltpu.CompilerParams(vmem_limit_bytes=20 << 20),
        name="ffn",
    )(total, left, right, *weights)


def own_down_kernel(hidden_ref, down_ref, down2_ref, out_ref):
    blocks, _, depth = out_ref.shape
    for b in range(0, blocks, 2):
        partial = down_pair(hidden_ref[...], (down_ref, down2_ref), b, class_at(0), depth)
        out_ref[b] = partial[:, :depth]
        out_ref[b + 1] = partial[:, depth:]


def own_down(hidden, down, down2):
    rows = hidden.shape[0]
    width, model = down.shape
    depth = model // (CLASSES * QUARTERS)
    return pl.pallas_call(
        own_down_kernel,
        out_shape=jax.ShapeDtypeStruct((QUARTERS, rows, depth), jnp.float32),
        cost_estimate=cost(rows * model * width, 4000000),
        compiler_params=pltpu.CompilerParams(vmem_limit_bytes=16 << 20),
        name="own_down",
    )(hidden, down, down2)


def join_kernel(own_ref, left_ref, right_ref, left2_ref, right2_ref, out_ref):
    blocks = own_ref.shape[0]
    chips = out_ref.shape[0]
    half = blocks // 2
    for q in range(blocks):
        both = own_ref[q] + left_ref[q].astype(jnp.float32) + right_ref[q].astype(jnp.float32)
        third = left2_ref[q] if q < half else right2_ref[q - half]
        both = (both + third.astype(jnp.float32)).astype(jnp.bfloat16)
        at = QUARTERS * MAIN + q * TAIL
        for chip in range(chips):
            tail = chips * MAIN + chip * TAIL
            out_ref[chip, q * MAIN : (q + 1) * MAIN] = both[chip * MAIN : (chip + 1) * MAIN]
            out_ref[chip, at : at + TAIL] = both[tail : tail + TAIL]


def join(own, left, right, left2, right2, chips):
    blocks, rows, depth = own.shape
    return pl.pallas_call(
        join_kernel,
        out_shape=jax.ShapeDtypeStruct((chips, blocks * CAP, depth), jnp.bfloat16),
        cost_estimate=cost(blocks * rows * depth, 12 * blocks * rows * depth),
        compiler_params=pltpu.CompilerParams(vmem_limit_bytes=16 << 20),
        name="join",
    )(own, left, right, left2, right2)


def combine_kernel(mix_ref, back_ref, out_ref):
    blocks, count, depth = out_ref.shape
    per_quarter = blocks // QUARTERS
    summed = lax.dot_general(
        mix_ref[...], back_ref[...], (((0,), (0,)), ((), ())), preferred_element_type=jnp.float32
    ).astype(jnp.bfloat16)
    for q in range(QUARTERS):
        for s in range(per_quarter):
            out_ref[q * per_quarter + s] = summed[
                q * count : (q + 1) * count, s * depth : (s + 1) * depth
            ]


def combine(mix, back, count, blocks):
    rows, quarter = back.shape
    depth = QUARTERS * quarter // blocks
    return pl.pallas_call(
        combine_kernel,
        out_shape=jax.ShapeDtypeStruct((blocks, count, depth), jnp.bfloat16),
        cost_estimate=cost(2 * rows * quarter * 128, 2400000),
        compiler_params=pltpu.CompilerParams(vmem_limit_bytes=12 << 20),
        name="combine",
    )(mix, back)


def on_device(tokens, expert_ids, route_logits, gate_weight, up_weight, down_weight):
    chips = lax.axis_size("x")
    pairs = lax.axis_size("quarter") * lax.axis_size("half")
    parts = 2 * pairs
    count, depth = tokens.shape
    swap = [(0, 1), (1, 0)]
    along = ("quarter", "half", "odd")
    ids = expert_ids.T

    def shift(value, distance):
        return lax.ppermute(value, along, [(i, (i + distance) % parts) for i in range(parts)])

    outgoing = dispatch(ids, tokens, chips)
    gate, up, outgoing = lax.optimization_barrier((gate_weight, up_weight, outgoing))
    incoming = lax.all_to_all(outgoing, "x", 0, 0, tiled=True)
    gate2 = lax.ppermute(gate, "core", swap)
    up2 = lax.ppermute(up, "core", swap)
    own = lax.all_gather(gather_rows(incoming), ("quarter", "half"))
    down, own = lax.optimization_barrier((down_weight, own))
    left = shift(own[: pairs // 2], 1)
    right = shift(own[pairs // 2 :], -1)
    down2 = lax.ppermute(down, "core", swap)
    blocks = [w.reshape(pairs, 2, depth, w.shape[1]) for w in (gate, gate2, up, up2)]
    total = own_part(own, *blocks)
    hidden, to_right, to_left, to_right2, to_left2 = ffn(total, left, right, *blocks, down, down2)
    left, right = shift(to_right, 1), shift(to_left, -1)
    left2, right2 = shift(to_right2, 2), shift(to_left2, -2)
    partial_value = join(own_down(hidden, down, down2), left, right, left2, right2, chips)
    returned = lax.all_to_all(partial_value, "x", 0, 0, tiled=True)
    mix = mixing(ids, route_logits.T, chips)
    combined = combine(mix, returned.reshape(chips * QUARTERS * CAP, depth), count, QUARTERS)
    blocks = lax.all_to_all(combined, "quarter", 0, 0, tiled=True)
    return jnp.sum(blocks.astype(jnp.float32), axis=0).astype(jnp.bfloat16)


def solution(mesh):
    sizes = [mesh.shape[axis] for axis in ("rep", "exp", "tp")]
    devices = mesh.devices.reshape(sizes[0], sizes[1] // CORES, CORES, QUARTERS, 2, 2)
    split = Mesh(devices, ("rep", "x", "core", "quarter", "half", "odd"))
    tokens = ("rep", "x", "core")
    features = ("quarter", "half", "odd")
    hidden = ("x", "core", "quarter", "half", "odd")
    return jax.shard_map(
        on_device,
        mesh=split,
        in_specs=(
            P(tokens, features),
            P(tokens, None),
            P(tokens, None),
            P(None, hidden),
            P(None, hidden),
            P(hidden, None),
        ),
        out_specs=P(tokens, features),
        check_vma=False,
    )
```

```python
import functools

import jax
import jax.numpy as jnp
from jax import lax
from jax.experimental import pallas as pl
from jax.experimental.pallas import tpu as pltpu
from jax.sharding import Mesh, PartitionSpec as P


EXPERTS = 4
CAP = 20
MAIN = 16
TAIL = CAP - MAIN
QUARTERS = 4
CORES = 2


def cost(flops, nbytes):
    return pl.CostEstimate(flops=flops, bytes_accessed=nbytes, transcendentals=0)


def count_at_least(index, width, parts):
    total = jnp.zeros_like(index)
    for k in range(1, parts):
        total = total + (index >= k * width).astype(jnp.int32)
    return total


def placed(ids, expert, slot, before):
    chosen = ((ids[0:1, :] == expert) | (ids[1:2, :] == expert)).astype(jnp.float32)
    position = jnp.dot(chosen, before, preferred_element_type=jnp.float32)
    return chosen * (position == slot.astype(jnp.float32)).astype(jnp.float32)


def grouped(row, groups):
    later = row >= groups * MAIN
    rest = row - groups * MAIN
    main = count_at_least(row, MAIN, groups)
    tail = count_at_least(rest, TAIL, groups)
    group = jnp.where(later, tail, main)
    slot = jnp.where(later, MAIN + rest - TAIL * tail, row - MAIN * main)
    return group, slot


def dispatch_kernel(chips, ids_ref, tokens_ref, out_ref):
    count = tokens_ref.shape[0]
    row = lax.broadcasted_iota(jnp.int32, (EXPERTS * CAP, count), 0)
    expert = count_at_least(row, CAP, EXPERTS)
    slot = row - CAP * expert
    first = lax.broadcasted_iota(jnp.int32, (count, count), 0)
    second = lax.broadcasted_iota(jnp.int32, (count, count), 1)
    before = (first < second).astype(jnp.float32)
    placement = placed(ids_ref[...], expert, slot, before).astype(jnp.bfloat16)
    slots = jnp.dot(placement, tokens_ref[...], preferred_element_type=jnp.float32).astype(
        jnp.bfloat16
    )
    per_expert = chips // EXPERTS
    for chip in range(chips):
        e = chip // per_expert
        out_ref[chip] = slots[e * CAP : (e + 1) * CAP]


def dispatch(ids, tokens, chips):
    count, features = tokens.shape
    return pl.pallas_call(
        functools.partial(dispatch_kernel, chips),
        out_shape=jax.ShapeDtypeStruct((chips, CAP, features), jnp.bfloat16),
        cost_estimate=cost(2 * EXPERTS * CAP * count * features, 200000),
        compiler_params=pltpu.CompilerParams(vmem_limit_bytes=60 << 20),
        name="dispatch",
    )(ids, tokens)


def gather_rows_kernel(in_ref, out_ref):
    chips = in_ref.shape[0]
    for chip in range(chips):
        out_ref[chip * MAIN : (chip + 1) * MAIN] = in_ref[chip, :MAIN]
        at = chips * MAIN + chip * TAIL
        out_ref[at : at + TAIL] = in_ref[chip, MAIN:]


def gather_rows(slots):
    chips, _, depth = slots.shape
    return pl.pallas_call(
        gather_rows_kernel,
        out_shape=jax.ShapeDtypeStruct((chips * CAP, depth), jnp.bfloat16),
        cost_estimate=cost(1000, 250000),
        compiler_params=pltpu.CompilerParams(vmem_limit_bytes=4 << 20),
        name="gather_rows",
    )(slots)


def mixing_kernel(chips, count, ids_ref, logits_ref, out_ref):
    lanes = ids_ref.shape[1]
    rows = chips * QUARTERS * CAP
    row = lax.broadcasted_iota(jnp.int32, (rows, lanes), 0)
    chip = count_at_least(row, QUARTERS * CAP, chips)
    quarter, slot = grouped(row - QUARTERS * CAP * chip, QUARTERS)
    expert = count_at_least(chip, chips // EXPERTS, EXPERTS)
    lane = lax.broadcasted_iota(jnp.int32, (rows, lanes), 1)
    own = (count_at_least(lane, count, QUARTERS) == quarter).astype(jnp.float32)
    first = lax.broadcasted_iota(jnp.int32, (lanes, lanes), 0)
    second = lax.broadcasted_iota(jnp.int32, (lanes, lanes), 1)
    same = count_at_least(first, count, QUARTERS) == count_at_least(second, count, QUARTERS)
    before = ((first < second) & same).astype(jnp.float32)
    ids = ids_ref[...]
    diff = logits_ref[0:1, :] - logits_ref[1:2, :]
    share = jnp.where(ids[0:1, :] == expert, jax.nn.sigmoid(diff), jax.nn.sigmoid(-diff))
    out_ref[...] = (placed(ids, expert, slot, before) * share * own).astype(jnp.bfloat16)


def mixing(ids, logits, chips):
    count = ids.shape[1]
    rows = chips * QUARTERS * CAP
    return pl.pallas_call(
        functools.partial(mixing_kernel, chips, count),
        out_shape=jax.ShapeDtypeStruct((rows, QUARTERS * count), jnp.bfloat16),
        cost_estimate=cost(2 * rows * 128 * 128, 200000),
        compiler_params=pltpu.CompilerParams(vmem_limit_bytes=8 << 20),
        name="mixing",
    )(jnp.tile(ids, (1, QUARTERS)), jnp.tile(logits, (1, QUARTERS)))


def side_by_side(refs, b, parity):
    return jnp.concatenate(
        [ref[b, parity if ref.shape[1] > 1 else 0] for ref in refs], axis=1
    )


def multiply(total, tokens, refs, parity, start):
    for b in range(0, tokens.shape[0], 2):
        rows = jnp.concatenate([tokens[b], tokens[b + 1]], axis=1)
        weight = jnp.concatenate(
            [side_by_side(refs, start + b, parity), side_by_side(refs, start + b + 1, parity)],
            axis=0,
        )
        added = jnp.dot(rows, weight, preferred_element_type=jnp.float32)
        total = added if total is None else total + added
    return total


def own_kernel(slots_ref, gate_ref, gate2_ref, up_ref, up2_ref, out_ref, rest_ref):
    refs = (gate_ref, gate2_ref, up_ref, up2_ref)
    parity = lax.axis_index("odd")
    out_ref[...] = multiply(None, slots_ref, refs, parity, 0)
    for b in range(slots_ref.shape[0]):
        rest_ref[b, 0] = up2_ref[b, 1 - parity]


def own_part(slots, *weights):
    pairs, rows, depth = slots.shape
    width = weights[0].shape[-1]
    return pl.pallas_call(
        own_kernel,
        out_shape=(
            jax.ShapeDtypeStruct((rows, 4 * width), jnp.float32),
            jax.ShapeDtypeStruct((pairs, 1, depth, width), jnp.bfloat16),
        ),
        cost_estimate=cost(2 * pairs * rows * depth * 4 * width, 4200000),
        compiler_params=pltpu.CompilerParams(vmem_limit_bytes=16 << 20),
        name="own_part",
    )(slots, *weights)


def down_pair(hidden, refs, b, parity, depth):
    def block(b):
        lanes = pl.ds(pl.multiple_of((2 * b + parity) * depth, 128), depth)
        return jnp.concatenate([ref[:, lanes] for ref in refs], axis=0)

    weight = jnp.concatenate([block(b), block(b + 1)], axis=1)
    return jnp.dot(hidden, weight, preferred_element_type=jnp.float32)


def ffn_kernel(
    total_ref, left_ref, right_ref, gate_ref, gate2_ref, up_ref, up2_ref, down_ref, down2_ref, hidden_ref, to_right_ref, to_left_ref
):
    half, _, depth = left_ref.shape
    parity = 1 - lax.axis_index("odd")
    width = gate_ref.shape[-1]
    refs = (gate_ref, gate2_ref, up_ref, up2_ref)
    total = multiply(total_ref[...], left_ref, refs, parity, 0)
    total = multiply(total, right_ref, refs, parity, half)
    gate = total[:, : 2 * width]
    hidden = (gate * jax.nn.sigmoid(gate) * total[:, 2 * width :]).astype(jnp.bfloat16)
    hidden_ref[...] = hidden
    for b in range(0, 2 * half, 2):
        partial = down_pair(hidden, (down_ref, down2_ref), b, parity, depth).astype(jnp.bfloat16)
        out_ref, at = (to_right_ref, b) if b < half else (to_left_ref, b - half)
        out_ref[at] = partial[:, :depth]
        out_ref[at + 1] = partial[:, depth:]


def ffn(total, left, right, *weights):
    _, rows, _ = left.shape
    width, model = weights[-1].shape
    sent = jax.ShapeDtypeStruct(left.shape, jnp.bfloat16)
    return pl.pallas_call(
        ffn_kernel,
        out_shape=(jax.ShapeDtypeStruct((rows, 2 * width), jnp.bfloat16), sent, sent),
        cost_estimate=cost(2 * rows * model * width * 3, 7000000),
        compiler_params=pltpu.CompilerParams(vmem_limit_bytes=20 << 20),
        name="ffn",
    )(total, left, right, *weights)


def own_down_kernel(hidden_ref, down_ref, down2_ref, out_ref):
    pairs, _, depth = out_ref.shape
    parity = lax.axis_index("odd")
    for b in range(0, pairs, 2):
        partial = down_pair(hidden_ref[...], (down_ref, down2_ref), b, parity, depth)
        out_ref[b] = partial[:, :depth]
        out_ref[b + 1] = partial[:, depth:]


def own_down(hidden, down, down2, pairs):
    rows = hidden.shape[0]
    width, model = down.shape
    depth = model // (2 * pairs)
    return pl.pallas_call(
        own_down_kernel,
        out_shape=jax.ShapeDtypeStruct((pairs, rows, depth), jnp.float32),
        cost_estimate=cost(2 * rows * model * width, 4000000),
        compiler_params=pltpu.CompilerParams(vmem_limit_bytes=16 << 20),
        name="own_down",
    )(hidden, down, down2)


def join_kernel(own_ref, left_ref, right_ref, out_ref):
    pairs, _, depth = own_ref.shape
    chips = out_ref.shape[0]
    half = pairs // 2
    per_quarter = pairs // QUARTERS
    for b in range(pairs):
        other = left_ref[b] if b < half else right_ref[b - half]
        both = (own_ref[b] + other.astype(jnp.float32)).astype(jnp.bfloat16)
        q, s = b // per_quarter, b % per_quarter
        at = QUARTERS * MAIN + q * TAIL
        lanes = slice(s * depth, (s + 1) * depth)
        for chip in range(chips):
            tail = chips * MAIN + chip * TAIL
            out_ref[chip, q * MAIN : (q + 1) * MAIN, lanes] = both[chip * MAIN : (chip + 1) * MAIN]
            out_ref[chip, at : at + TAIL, lanes] = both[tail : tail + TAIL]


def join(own, left, right, chips):
    pairs, rows, depth = own.shape
    out = (chips, QUARTERS * CAP, pairs * depth // QUARTERS)
    return pl.pallas_call(
        join_kernel,
        out_shape=jax.ShapeDtypeStruct(out, jnp.bfloat16),
        cost_estimate=cost(pairs * rows * depth, 8 * pairs * rows * depth),
        compiler_params=pltpu.CompilerParams(vmem_limit_bytes=16 << 20),
        name="join",
    )(own, left, right)


def combine_kernel(mix_ref, back_ref, out_ref):
    blocks, count, depth = out_ref.shape
    per_quarter = blocks // QUARTERS
    summed = lax.dot_general(
        mix_ref[...], back_ref[...], (((0,), (0,)), ((), ())), preferred_element_type=jnp.float32
    ).astype(jnp.bfloat16)
    for q in range(QUARTERS):
        for s in range(per_quarter):
            out_ref[q * per_quarter + s] = summed[
                q * count : (q + 1) * count, s * depth : (s + 1) * depth
            ]


def combine(mix, back, count, blocks):
    rows, quarter = back.shape
    depth = QUARTERS * quarter // blocks
    return pl.pallas_call(
        combine_kernel,
        out_shape=jax.ShapeDtypeStruct((blocks, count, depth), jnp.bfloat16),
        cost_estimate=cost(2 * rows * quarter * 128, 2400000),
        compiler_params=pltpu.CompilerParams(vmem_limit_bytes=12 << 20),
        name="combine",
    )(mix, back)


def on_device(tokens, expert_ids, route_logits, gate_weight, up_weight, down_weight):
    chips = lax.axis_size("x")
    pairs = lax.axis_size("pair")
    parts = 2 * pairs
    count, depth = tokens.shape
    swap = [(0, 1), (1, 0)]
    along = ("pair", "odd")
    ids = expert_ids.T
    up_z = [(i, (i + 1) % parts) for i in range(parts)]
    down_z = [((i + 1) % parts, i) for i in range(parts)]
    outgoing = dispatch(ids, tokens, chips)
    gate, up, down, outgoing = lax.optimization_barrier(
        (gate_weight, up_weight, down_weight, outgoing)
    )
    incoming = lax.all_to_all(outgoing, "x", 0, 0, tiled=True)
    gate2 = lax.ppermute(gate, "core", swap)
    up2 = lax.ppermute(up, "core", swap)
    down2 = lax.ppermute(down, "core", swap)
    own = lax.all_gather(gather_rows(incoming), "pair")
    left = lax.ppermute(own[: pairs // 2], along, up_z)
    right = lax.ppermute(own[pairs // 2 :], along, down_z)
    blocks = [w.reshape(pairs, 2, depth, w.shape[1]) for w in (gate, gate2, up, up2)]
    total, rest = own_part(own, *blocks)
    hidden, to_right, to_left = ffn(total, left, right, *blocks[:3], rest, down, down2)
    from_left = lax.ppermute(to_right, along, up_z)
    from_right = lax.ppermute(to_left, along, down_z)
    partial_value = join(own_down(hidden, down, down2, pairs), from_left, from_right, chips)
    returned = lax.all_to_all(partial_value, "x", 0, 0, tiled=True)
    mix = mixing(ids, route_logits.T, chips)
    back = returned.reshape(chips * QUARTERS * CAP, pairs * depth // QUARTERS)
    combined = combine(mix, back, count, pairs)
    blocks = lax.all_to_all(combined, "pair", 0, 0, tiled=True)
    return jnp.sum(blocks.astype(jnp.float32), axis=0).astype(jnp.bfloat16)


def solution(mesh):
    sizes = [mesh.shape[axis] for axis in ("rep", "exp", "tp")]
    devices = mesh.devices.reshape(sizes[0], sizes[1] // CORES, CORES, sizes[2] // 2, 2)
    split = Mesh(devices, ("rep", "x", "core", "pair", "odd"))
    tokens = ("rep", "x", "core")
    features = ("pair", "odd")
    hidden = ("x", "core", "pair", "odd")
    return jax.shard_map(
        on_device,
        mesh=split,
        in_specs=(
            P(tokens, features),
            P(tokens, None),
            P(tokens, None),
            P(None, hidden),
            P(None, hidden),
            P(hidden, None),
        ),
        out_specs=P(tokens, features),
        check_vma=False,
    )
```

```python
import functools

import jax
import jax.numpy as jnp
from jax import lax
from jax.experimental import pallas as pl
from jax.experimental.pallas import tpu as pltpu
from jax.sharding import Mesh, PartitionSpec as P


EXPERTS = 4
CAP = 20
MAIN = 16
TAIL = CAP - MAIN
QUARTERS = 4
CLASSES = 4
CORES = 2


def cost(flops, nbytes):
    return pl.CostEstimate(flops=flops, bytes_accessed=nbytes, transcendentals=0)


def count_at_least(index, width, parts):
    total = jnp.zeros_like(index)
    for k in range(1, parts):
        total = total + (index >= k * width).astype(jnp.int32)
    return total


def placed(ids, expert, slot, before):
    chosen = ((ids[0:1, :] == expert) | (ids[1:2, :] == expert)).astype(jnp.float32)
    position = jnp.dot(chosen, before, preferred_element_type=jnp.float32)
    return chosen * (position == slot.astype(jnp.float32)).astype(jnp.float32)


def grouped(row, groups):
    later = row >= groups * MAIN
    rest = row - groups * MAIN
    main = count_at_least(row, MAIN, groups)
    tail = count_at_least(rest, TAIL, groups)
    group = jnp.where(later, tail, main)
    slot = jnp.where(later, MAIN + rest - TAIL * tail, row - MAIN * main)
    return group, slot


def dispatch_kernel(chips, ids_ref, tokens_ref, out_ref):
    count = tokens_ref.shape[0]
    row = lax.broadcasted_iota(jnp.int32, (EXPERTS * CAP, count), 0)
    expert = count_at_least(row, CAP, EXPERTS)
    slot = row - CAP * expert
    first = lax.broadcasted_iota(jnp.int32, (count, count), 0)
    second = lax.broadcasted_iota(jnp.int32, (count, count), 1)
    before = (first < second).astype(jnp.float32)
    placement = placed(ids_ref[...], expert, slot, before).astype(jnp.bfloat16)
    slots = jnp.dot(placement, tokens_ref[...], preferred_element_type=jnp.float32).astype(
        jnp.bfloat16
    )
    per_expert = chips // EXPERTS
    for chip in range(chips):
        e = chip // per_expert
        out_ref[chip] = slots[e * CAP : (e + 1) * CAP]


def dispatch(ids, tokens, chips):
    count, features = tokens.shape
    return pl.pallas_call(
        functools.partial(dispatch_kernel, chips),
        out_shape=jax.ShapeDtypeStruct((chips, CAP, features), jnp.bfloat16),
        cost_estimate=cost(2 * EXPERTS * CAP * count * features, 200000),
        compiler_params=pltpu.CompilerParams(vmem_limit_bytes=60 << 20),
        name="dispatch",
    )(ids, tokens)


def gather_rows_kernel(in_ref, out_ref):
    chips = in_ref.shape[0]
    for chip in range(chips):
        out_ref[chip * MAIN : (chip + 1) * MAIN] = in_ref[chip, :MAIN]
        at = chips * MAIN + chip * TAIL
        out_ref[at : at + TAIL] = in_ref[chip, MAIN:]


def gather_rows(slots):
    chips, _, depth = slots.shape
    return pl.pallas_call(
        gather_rows_kernel,
        out_shape=jax.ShapeDtypeStruct((chips * CAP, depth), jnp.bfloat16),
        cost_estimate=cost(1000, 250000),
        compiler_params=pltpu.CompilerParams(vmem_limit_bytes=4 << 20),
        name="gather_rows",
    )(slots)


def mixing_kernel(chips, count, ids_ref, logits_ref, out_ref):
    lanes = ids_ref.shape[1]
    rows = chips * QUARTERS * CAP
    row = lax.broadcasted_iota(jnp.int32, (rows, lanes), 0)
    chip = count_at_least(row, QUARTERS * CAP, chips)
    quarter, slot = grouped(row - QUARTERS * CAP * chip, QUARTERS)
    expert = count_at_least(chip, chips // EXPERTS, EXPERTS)
    lane = lax.broadcasted_iota(jnp.int32, (rows, lanes), 1)
    own = (count_at_least(lane, count, QUARTERS) == quarter).astype(jnp.float32)
    first = lax.broadcasted_iota(jnp.int32, (lanes, lanes), 0)
    second = lax.broadcasted_iota(jnp.int32, (lanes, lanes), 1)
    same = count_at_least(first, count, QUARTERS) == count_at_least(second, count, QUARTERS)
    before = ((first < second) & same).astype(jnp.float32)
    ids = ids_ref[...]
    diff = logits_ref[0:1, :] - logits_ref[1:2, :]
    share = jnp.where(ids[0:1, :] == expert, jax.nn.sigmoid(diff), jax.nn.sigmoid(-diff))
    out_ref[...] = (placed(ids, expert, slot, before) * share * own).astype(jnp.bfloat16)


def mixing(ids, logits, chips):
    count = ids.shape[1]
    rows = chips * QUARTERS * CAP
    return pl.pallas_call(
        functools.partial(mixing_kernel, chips, count),
        out_shape=jax.ShapeDtypeStruct((rows, QUARTERS * count), jnp.bfloat16),
        cost_estimate=cost(2 * rows * 128 * 128, 200000),
        compiler_params=pltpu.CompilerParams(vmem_limit_bytes=8 << 20),
        name="mixing",
    )(jnp.tile(ids, (1, QUARTERS)), jnp.tile(logits, (1, QUARTERS)))


def class_at(distance):
    own = 2 * lax.axis_index("half") + lax.axis_index("odd")
    return lax.rem(own + CLASSES + distance, CLASSES)


def side_by_side(refs, b, parity):
    return jnp.concatenate(
        [ref[b, parity if ref.shape[1] > 1 else 0] for ref in refs], axis=1
    )


def multiply(total, tokens, refs, parity, start):
    for b in range(0, tokens.shape[0], 2):
        rows = jnp.concatenate([tokens[b], tokens[b + 1]], axis=1)
        weight = jnp.concatenate(
            [side_by_side(refs, start + b, parity), side_by_side(refs, start + b + 1, parity)],
            axis=0,
        )
        added = jnp.dot(rows, weight, preferred_element_type=jnp.float32)
        total = added if total is None else total + added
    return total


def own_kernel(slots_ref, gate_ref, gate2_ref, up_ref, up2_ref, out_ref, rest_ref):
    refs = (gate_ref, gate2_ref, up_ref, up2_ref)
    parity = lax.axis_index("odd")
    out_ref[...] = multiply(None, slots_ref, refs, parity, 0)
    for b in range(slots_ref.shape[0]):
        rest_ref[b, 0] = up2_ref[b, 1 - parity]


def own_part(slots, *weights):
    pairs, rows, depth = slots.shape
    width = weights[0].shape[-1]
    return pl.pallas_call(
        own_kernel,
        out_shape=(
            jax.ShapeDtypeStruct((rows, 4 * width), jnp.float32),
            jax.ShapeDtypeStruct((pairs, 1, depth, width), jnp.bfloat16),
        ),
        cost_estimate=cost(2 * pairs * rows * depth * 4 * width, 4200000),
        compiler_params=pltpu.CompilerParams(vmem_limit_bytes=16 << 20),
        name="own_part",
    )(slots, *weights)


def down_pair(hidden, refs, q, kind, depth):
    def block(q):
        lanes = pl.ds(pl.multiple_of((CLASSES * q + kind) * depth, 128), depth)
        return jnp.concatenate([ref[:, lanes] for ref in refs], axis=0)

    weight = jnp.concatenate([block(q), block(q + 1)], axis=1)
    return jnp.dot(hidden, weight, preferred_element_type=jnp.float32)


def ffn_kernel(
    total_ref, left_ref, right_ref, gate_ref, gate2_ref, up_ref, up2_ref, down_ref, down2_ref, hidden_ref, to_right_ref, to_left_ref, to_right2_ref, to_left2_ref
):
    pairs, _, depth = left_ref.shape
    parity = 1 - lax.axis_index("odd")
    width = gate_ref.shape[-1]
    half = QUARTERS // 2
    refs = (gate_ref, gate2_ref, up_ref, up2_ref)
    total = multiply(total_ref[...], left_ref, refs, parity, 0)
    total = multiply(total, right_ref, refs, parity, pairs)
    gate = total[:, : 2 * width]
    hidden = (gate * jax.nn.sigmoid(gate) * total[:, 2 * width :]).astype(jnp.bfloat16)
    hidden_ref[...] = hidden
    downs = (down_ref, down2_ref)
    for out_ref, distance, start in (
        (to_right_ref, 1, 0),
        (to_left_ref, -1, 0),
        (to_right2_ref, 2, 0),
        (to_left2_ref, 2, half),
    ):
        for b in range(0, out_ref.shape[0], 2):
            partial = down_pair(hidden, downs, start + b, class_at(distance), depth)
            partial = partial.astype(jnp.bfloat16)
            out_ref[b] = partial[:, :depth]
            out_ref[b + 1] = partial[:, depth:]


def ffn(total, left, right, *weights):
    rows, depth = left.shape[1:]
    width, model = weights[-1].shape
    sent = jax.ShapeDtypeStruct((QUARTERS, rows, depth), jnp.bfloat16)
    half = jax.ShapeDtypeStruct((QUARTERS // 2, rows, depth), jnp.bfloat16)
    return pl.pallas_call(
        ffn_kernel,
        out_shape=(
            jax.ShapeDtypeStruct((rows, 2 * width), jnp.bfloat16),
            sent,
            sent,
            half,
            half,
        ),
        cost_estimate=cost(2 * rows * model * width * 4, 9000000),
        compiler_params=pltpu.CompilerParams(vmem_limit_bytes=20 << 20),
        name="ffn",
    )(total, left, right, *weights)


def own_down_kernel(hidden_ref, down_ref, down2_ref, out_ref):
    blocks, _, depth = out_ref.shape
    for b in range(0, blocks, 2):
        partial = down_pair(hidden_ref[...], (down_ref, down2_ref), b, class_at(0), depth)
        out_ref[b] = partial[:, :depth]
        out_ref[b + 1] = partial[:, depth:]


def own_down(hidden, down, down2):
    rows = hidden.shape[0]
    width, model = down.shape
    depth = model // (CLASSES * QUARTERS)
    return pl.pallas_call(
        own_down_kernel,
        out_shape=jax.ShapeDtypeStruct((QUARTERS, rows, depth), jnp.float32),
        cost_estimate=cost(rows * model * width, 4000000),
        compiler_params=pltpu.CompilerParams(vmem_limit_bytes=16 << 20),
        name="own_down",
    )(hidden, down, down2)


def join_kernel(own_ref, left_ref, right_ref, left2_ref, right2_ref, out_ref):
    blocks = own_ref.shape[0]
    chips = out_ref.shape[0]
    half = blocks // 2
    for q in range(blocks):
        both = own_ref[q] + left_ref[q].astype(jnp.float32) + right_ref[q].astype(jnp.float32)
        third = left2_ref[q] if q < half else right2_ref[q - half]
        both = (both + third.astype(jnp.float32)).astype(jnp.bfloat16)
        at = QUARTERS * MAIN + q * TAIL
        for chip in range(chips):
            tail = chips * MAIN + chip * TAIL
            out_ref[chip, q * MAIN : (q + 1) * MAIN] = both[chip * MAIN : (chip + 1) * MAIN]
            out_ref[chip, at : at + TAIL] = both[tail : tail + TAIL]


def join(own, left, right, left2, right2, chips):
    blocks, rows, depth = own.shape
    return pl.pallas_call(
        join_kernel,
        out_shape=jax.ShapeDtypeStruct((chips, blocks * CAP, depth), jnp.bfloat16),
        cost_estimate=cost(blocks * rows * depth, 12 * blocks * rows * depth),
        compiler_params=pltpu.CompilerParams(vmem_limit_bytes=16 << 20),
        name="join",
    )(own, left, right, left2, right2)


def combine_kernel(mix_ref, back_ref, out_ref):
    blocks, count, depth = out_ref.shape
    per_quarter = blocks // QUARTERS
    summed = lax.dot_general(
        mix_ref[...], back_ref[...], (((0,), (0,)), ((), ())), preferred_element_type=jnp.float32
    ).astype(jnp.bfloat16)
    for q in range(QUARTERS):
        for s in range(per_quarter):
            out_ref[q * per_quarter + s] = summed[
                q * count : (q + 1) * count, s * depth : (s + 1) * depth
            ]


def combine(mix, back, count, blocks):
    rows, quarter = back.shape
    depth = QUARTERS * quarter // blocks
    return pl.pallas_call(
        combine_kernel,
        out_shape=jax.ShapeDtypeStruct((blocks, count, depth), jnp.bfloat16),
        cost_estimate=cost(2 * rows * quarter * 128, 2400000),
        compiler_params=pltpu.CompilerParams(vmem_limit_bytes=12 << 20),
        name="combine",
    )(mix, back)


def on_device(tokens, expert_ids, route_logits, gate_weight, up_weight, down_weight):
    chips = lax.axis_size("x")
    pairs = lax.axis_size("quarter") * lax.axis_size("half")
    parts = 2 * pairs
    count, depth = tokens.shape
    swap = [(0, 1), (1, 0)]
    along = ("quarter", "half", "odd")
    ids = expert_ids.T

    def shift(value, distance):
        return lax.ppermute(value, along, [(i, (i + distance) % parts) for i in range(parts)])

    outgoing = dispatch(ids, tokens, chips)
    gate, up, down, outgoing = lax.optimization_barrier(
        (gate_weight, up_weight, down_weight, outgoing)
    )
    incoming = lax.all_to_all(outgoing, "x", 0, 0, tiled=True)
    gate2 = lax.ppermute(gate, "core", swap)
    up2 = lax.ppermute(up, "core", swap)
    down2 = lax.ppermute(down, "core", swap)
    own = lax.all_gather(gather_rows(incoming), ("quarter", "half"))
    left, right = shift(own[: pairs // 2], 1), shift(own[pairs // 2 :], -1)
    blocks = [w.reshape(pairs, 2, depth, w.shape[1]) for w in (gate, gate2, up, up2)]
    total, rest = own_part(own, *blocks)
    hidden, to_right, to_left, to_right2, to_left2 = ffn(
        total, left, right, *blocks[:3], rest, down, down2
    )
    left, right = shift(to_right, 1), shift(to_left, -1)
    left2, right2 = shift(to_right2, 2), shift(to_left2, -2)
    partial_value = join(own_down(hidden, down, down2), left, right, left2, right2, chips)
    returned = lax.all_to_all(partial_value, "x", 0, 0, tiled=True)
    mix = mixing(ids, route_logits.T, chips)
    combined = combine(mix, returned.reshape(chips * QUARTERS * CAP, depth), count, QUARTERS)
    blocks = lax.all_to_all(combined, "quarter", 0, 0, tiled=True)
    return jnp.sum(blocks.astype(jnp.float32), axis=0).astype(jnp.bfloat16)


def solution(mesh):
    sizes = [mesh.shape[axis] for axis in ("rep", "exp", "tp")]
    devices = mesh.devices.reshape(sizes[0], sizes[1] // CORES, CORES, QUARTERS, 2, 2)
    split = Mesh(devices, ("rep", "x", "core", "quarter", "half", "odd"))
    tokens = ("rep", "x", "core")
    features = ("quarter", "half", "odd")
    hidden = ("x", "core", "quarter", "half", "odd")
    return jax.shard_map(
        on_device,
        mesh=split,
        in_specs=(
            P(tokens, features),
            P(tokens, None),
            P(tokens, None),
            P(None, hidden),
            P(None, hidden),
            P(hidden, None),
        ),
        out_specs=P(tokens, features),
        check_vma=False,
    )
```

```python
import functools

import jax
import jax.numpy as jnp
from jax import lax
from jax.experimental import pallas as pl
from jax.experimental.pallas import tpu as pltpu
from jax.sharding import Mesh, PartitionSpec as P


EXPERTS = 4
CAP = 20
MAIN = 16
TAIL = CAP - MAIN
QUARTERS = 4
CLASSES = 4
CORES = 2


def cost(flops, nbytes):
    return pl.CostEstimate(flops=flops, bytes_accessed=nbytes, transcendentals=0)


def count_at_least(index, width, parts):
    total = jnp.zeros_like(index)
    for k in range(1, parts):
        total = total + (index >= k * width).astype(jnp.int32)
    return total


def placed(ids, expert, slot, before):
    chosen = ((ids[0:1, :] == expert) | (ids[1:2, :] == expert)).astype(jnp.float32)
    position = jnp.dot(chosen, before, preferred_element_type=jnp.float32)
    return chosen * (position == slot.astype(jnp.float32)).astype(jnp.float32)


def grouped(row, groups):
    later = row >= groups * MAIN
    rest = row - groups * MAIN
    main = count_at_least(row, MAIN, groups)
    tail = count_at_least(rest, TAIL, groups)
    group = jnp.where(later, tail, main)
    slot = jnp.where(later, MAIN + rest - TAIL * tail, row - MAIN * main)
    return group, slot


def dispatch_kernel(chips, ids_ref, tokens_ref, out_ref):
    count = tokens_ref.shape[0]
    row = lax.broadcasted_iota(jnp.int32, (EXPERTS * CAP, count), 0)
    expert = count_at_least(row, CAP, EXPERTS)
    slot = row - CAP * expert
    first = lax.broadcasted_iota(jnp.int32, (count, count), 0)
    second = lax.broadcasted_iota(jnp.int32, (count, count), 1)
    before = (first < second).astype(jnp.float32)
    placement = placed(ids_ref[...], expert, slot, before).astype(jnp.bfloat16)
    slots = jnp.dot(placement, tokens_ref[...], preferred_element_type=jnp.float32).astype(
        jnp.bfloat16
    )
    per_expert = chips // EXPERTS
    for chip in range(chips):
        e = chip // per_expert
        out_ref[chip] = slots[e * CAP : (e + 1) * CAP]


def dispatch(ids, tokens, chips):
    count, features = tokens.shape
    return pl.pallas_call(
        functools.partial(dispatch_kernel, chips),
        out_shape=jax.ShapeDtypeStruct((chips, CAP, features), jnp.bfloat16),
        cost_estimate=cost(2 * EXPERTS * CAP * count * features, 200000),
        compiler_params=pltpu.CompilerParams(vmem_limit_bytes=60 << 20),
        name="dispatch",
    )(ids, tokens)


def gather_rows_kernel(in_ref, out_ref):
    chips = in_ref.shape[0]
    for chip in range(chips):
        out_ref[chip * MAIN : (chip + 1) * MAIN] = in_ref[chip, :MAIN]
        at = chips * MAIN + chip * TAIL
        out_ref[at : at + TAIL] = in_ref[chip, MAIN:]


def gather_rows(slots):
    chips, _, depth = slots.shape
    return pl.pallas_call(
        gather_rows_kernel,
        out_shape=jax.ShapeDtypeStruct((chips * CAP, depth), jnp.bfloat16),
        cost_estimate=cost(1000, 250000),
        compiler_params=pltpu.CompilerParams(vmem_limit_bytes=4 << 20),
        name="gather_rows",
    )(slots)


def mixing_kernel(chips, count, ids_ref, logits_ref, out_ref):
    lanes = ids_ref.shape[1]
    rows = chips * QUARTERS * CAP
    row = lax.broadcasted_iota(jnp.int32, (rows, lanes), 0)
    chip = count_at_least(row, QUARTERS * CAP, chips)
    quarter, slot = grouped(row - QUARTERS * CAP * chip, QUARTERS)
    expert = count_at_least(chip, chips // EXPERTS, EXPERTS)
    lane = lax.broadcasted_iota(jnp.int32, (rows, lanes), 1)
    own = (count_at_least(lane, count, QUARTERS) == quarter).astype(jnp.float32)
    first = lax.broadcasted_iota(jnp.int32, (lanes, lanes), 0)
    second = lax.broadcasted_iota(jnp.int32, (lanes, lanes), 1)
    same = count_at_least(first, count, QUARTERS) == count_at_least(second, count, QUARTERS)
    before = ((first < second) & same).astype(jnp.float32)
    ids = ids_ref[...]
    diff = logits_ref[0:1, :] - logits_ref[1:2, :]
    share = jnp.where(ids[0:1, :] == expert, jax.nn.sigmoid(diff), jax.nn.sigmoid(-diff))
    out_ref[...] = (placed(ids, expert, slot, before) * share * own).astype(jnp.bfloat16)


def mixing(ids, logits, chips):
    count = ids.shape[1]
    rows = chips * QUARTERS * CAP
    return pl.pallas_call(
        functools.partial(mixing_kernel, chips, count),
        out_shape=jax.ShapeDtypeStruct((rows, QUARTERS * count), jnp.bfloat16),
        cost_estimate=cost(2 * rows * 128 * 128, 200000),
        compiler_params=pltpu.CompilerParams(vmem_limit_bytes=8 << 20),
        name="mixing",
    )(jnp.tile(ids, (1, QUARTERS)), jnp.tile(logits, (1, QUARTERS)))


def class_at(distance):
    own = 2 * lax.axis_index("half") + lax.axis_index("odd")
    return lax.rem(own + CLASSES + distance, CLASSES)


def side_by_side(refs, b, parity):
    return jnp.concatenate(
        [ref[b, parity if ref.shape[1] > 1 else 0] for ref in refs], axis=1
    )


def multiply(total, tokens, refs, parity, start):
    for b in range(0, tokens.shape[0], 2):
        rows = jnp.concatenate([tokens[b], tokens[b + 1]], axis=1)
        weight = jnp.concatenate(
            [side_by_side(refs, start + b, parity), side_by_side(refs, start + b + 1, parity)],
            axis=0,
        )
        added = jnp.dot(rows, weight, preferred_element_type=jnp.float32)
        total = added if total is None else total + added
    return total


def own_kernel(slots_ref, gate_ref, gate2_ref, up_ref, up2_ref, out_ref, rest_ref):
    refs = (gate_ref, gate2_ref, up_ref, up2_ref)
    parity = lax.axis_index("odd")
    out_ref[...] = multiply(None, slots_ref, refs, parity, 0)
    for b in range(slots_ref.shape[0]):
        rest_ref[b, 0] = up2_ref[b, 1 - parity]


def own_part(slots, *weights):
    pairs, rows, depth = slots.shape
    width = weights[0].shape[-1]
    return pl.pallas_call(
        own_kernel,
        out_shape=(
            jax.ShapeDtypeStruct((rows, 4 * width), jnp.float32),
            jax.ShapeDtypeStruct((pairs, 1, depth, width), jnp.bfloat16),
        ),
        cost_estimate=cost(2 * pairs * rows * depth * 4 * width, 4200000),
        compiler_params=pltpu.CompilerParams(vmem_limit_bytes=16 << 20),
        name="own_part",
    )(slots, *weights)


def down_pair(hidden, refs, q, kind, depth):
    def block(q):
        lanes = pl.ds(pl.multiple_of((CLASSES * q + kind) * depth, 128), depth)
        return jnp.concatenate([ref[:, lanes] for ref in refs], axis=0)

    weight = jnp.concatenate([block(q), block(q + 1)], axis=1)
    return jnp.dot(hidden, weight, preferred_element_type=jnp.float32)


def ffn_kernel(
    total_ref, left_ref, right_ref, gate_ref, gate2_ref, up_ref, up2_ref, down_ref, down2_ref, hidden_ref, to_right_ref, to_left_ref, to_right2_ref, to_left2_ref
):
    pairs, _, depth = left_ref.shape
    parity = 1 - lax.axis_index("odd")
    width = gate_ref.shape[-1]
    half = QUARTERS // 2
    refs = (gate_ref, gate2_ref, up_ref, up2_ref)
    total = multiply(total_ref[...], left_ref, refs, parity, 0)
    total = multiply(total, right_ref, refs, parity, pairs)
    gate = total[:, : 2 * width]
    hidden = (gate * jax.nn.sigmoid(gate) * total[:, 2 * width :]).astype(jnp.bfloat16)
    hidden_ref[...] = hidden
    downs = (down_ref, down2_ref)
    for out_ref, distance, start in (
        (to_right_ref, 1, 0),
        (to_left_ref, -1, 0),
        (to_right2_ref, 2, 0),
        (to_left2_ref, 2, half),
    ):
        for b in range(0, out_ref.shape[0], 2):
            partial = down_pair(hidden, downs, start + b, class_at(distance), depth)
            partial = partial.astype(jnp.bfloat16)
            out_ref[b] = partial[:, :depth]
            out_ref[b + 1] = partial[:, depth:]


def ffn(total, left, right, *weights):
    rows, depth = left.shape[1:]
    width, model = weights[-1].shape
    sent = jax.ShapeDtypeStruct((QUARTERS, rows, depth), jnp.bfloat16)
    half = jax.ShapeDtypeStruct((QUARTERS // 2, rows, depth), jnp.bfloat16)
    return pl.pallas_call(
        ffn_kernel,
        out_shape=(
            jax.ShapeDtypeStruct((rows, 2 * width), jnp.bfloat16),
            sent,
            sent,
            half,
            half,
        ),
        cost_estimate=cost(2 * rows * model * width * 4, 9000000),
        compiler_params=pltpu.CompilerParams(vmem_limit_bytes=20 << 20),
        name="ffn",
    )(total, left, right, *weights)


def own_down_kernel(hidden_ref, down_ref, down2_ref, out_ref):
    blocks, _, depth = out_ref.shape
    for b in range(0, blocks, 2):
        partial = down_pair(hidden_ref[...], (down_ref, down2_ref), b, class_at(0), depth)
        out_ref[b] = partial[:, :depth]
        out_ref[b + 1] = partial[:, depth:]


def own_down(hidden, down, down2):
    rows = hidden.shape[0]
    width, model = down.shape
    depth = model // (CLASSES * QUARTERS)
    return pl.pallas_call(
        own_down_kernel,
        out_shape=jax.ShapeDtypeStruct((QUARTERS, rows, depth), jnp.float32),
        cost_estimate=cost(rows * model * width, 4000000),
        compiler_params=pltpu.CompilerParams(vmem_limit_bytes=16 << 20),
        name="own_down",
    )(hidden, down, down2)


def join_kernel(own_ref, left_ref, right_ref, left2_ref, right2_ref, out_ref):
    blocks = own_ref.shape[0]
    chips = out_ref.shape[0]
    half = blocks // 2
    for q in range(blocks):
        both = own_ref[q] + left_ref[q].astype(jnp.float32) + right_ref[q].astype(jnp.float32)
        third = left2_ref[q] if q < half else right2_ref[q - half]
        both = (both + third.astype(jnp.float32)).astype(jnp.bfloat16)
        at = QUARTERS * MAIN + q * TAIL
        for chip in range(chips):
            tail = chips * MAIN + chip * TAIL
            out_ref[chip, q * MAIN : (q + 1) * MAIN] = both[chip * MAIN : (chip + 1) * MAIN]
            out_ref[chip, at : at + TAIL] = both[tail : tail + TAIL]


def join(own, left, right, left2, right2, chips):
    blocks, rows, depth = own.shape
    return pl.pallas_call(
        join_kernel,
        out_shape=jax.ShapeDtypeStruct((chips, blocks * CAP, depth), jnp.bfloat16),
        cost_estimate=cost(blocks * rows * depth, 12 * blocks * rows * depth),
        compiler_params=pltpu.CompilerParams(vmem_limit_bytes=16 << 20),
        name="join",
    )(own, left, right, left2, right2)


def combine_kernel(mix_ref, back_ref, out_ref):
    blocks, count, depth = out_ref.shape
    per_quarter = blocks // QUARTERS
    summed = lax.dot_general(
        mix_ref[...], back_ref[...], (((0,), (0,)), ((), ())), preferred_element_type=jnp.float32
    ).astype(jnp.bfloat16)
    for q in range(QUARTERS):
        for s in range(per_quarter):
            out_ref[q * per_quarter + s] = summed[
                q * count : (q + 1) * count, s * depth : (s + 1) * depth
            ]


def combine(mix, back, count, blocks):
    rows, quarter = back.shape
    depth = QUARTERS * quarter // blocks
    return pl.pallas_call(
        combine_kernel,
        out_shape=jax.ShapeDtypeStruct((blocks, count, depth), jnp.bfloat16),
        cost_estimate=cost(2 * rows * quarter * 128, 2400000),
        compiler_params=pltpu.CompilerParams(vmem_limit_bytes=12 << 20),
        name="combine",
    )(mix, back)


def on_device(tokens, expert_ids, route_logits, gate_weight, up_weight, down_weight):
    chips = lax.axis_size("x")
    pairs = lax.axis_size("quarter") * lax.axis_size("half")
    parts = 2 * pairs
    count, depth = tokens.shape
    swap = [(0, 1), (1, 0)]
    along = ("quarter", "half", "odd")
    ids = expert_ids.T

    def shift(value, distance):
        return lax.ppermute(value, along, [(i, (i + distance) % parts) for i in range(parts)])

    outgoing = dispatch(ids, tokens, chips)
    gate, up, down, outgoing = lax.optimization_barrier(
        (gate_weight, up_weight, down_weight, outgoing)
    )
    incoming = lax.all_to_all(outgoing, "x", 0, 0, tiled=True)
    gate2 = lax.ppermute(gate, "core", swap)
    up2 = lax.ppermute(up, "core", swap)
    down2 = lax.ppermute(down, "core", swap)
    own = lax.all_gather(gather_rows(incoming), ("quarter", "half"))
    left, right = shift(own[: pairs // 2], 1), shift(own[pairs // 2 :], -1)
    blocks = [w.reshape(pairs, 2, depth, w.shape[1]) for w in (gate, gate2, up, up2)]
    total, rest = own_part(own, *blocks)
    hidden, to_right, to_left, to_right2, to_left2 = ffn(
        total, left, right, *blocks[:3], rest, down, down2
    )
    left2 = shift(to_right2, 2)
    right2 = shift(to_left2, -2)
    left = shift(to_right, 1)
    right = shift(to_left, -1)
    partial_value = join(own_down(hidden, down, down2), left, right, left2, right2, chips)
    returned = lax.all_to_all(partial_value, "x", 0, 0, tiled=True)
    mix = mixing(ids, route_logits.T, chips)
    combined = combine(mix, returned.reshape(chips * QUARTERS * CAP, depth), count, QUARTERS)
    blocks = lax.all_to_all(combined, "quarter", 0, 0, tiled=True)
    return jnp.sum(blocks.astype(jnp.float32), axis=0).astype(jnp.bfloat16)


def solution(mesh):
    sizes = [mesh.shape[axis] for axis in ("rep", "exp", "tp")]
    devices = mesh.devices.reshape(sizes[0], sizes[1] // CORES, CORES, QUARTERS, 2, 2)
    split = Mesh(devices, ("rep", "x", "core", "quarter", "half", "odd"))
    tokens = ("rep", "x", "core")
    features = ("quarter", "half", "odd")
    hidden = ("x", "core", "quarter", "half", "odd")
    return jax.shard_map(
        on_device,
        mesh=split,
        in_specs=(
            P(tokens, features),
            P(tokens, None),
            P(tokens, None),
            P(None, hidden),
            P(None, hidden),
            P(hidden, None),
        ),
        out_specs=P(tokens, features),
        check_vma=False,
    )
```

```python
import functools

import jax
import jax.numpy as jnp
from jax import lax
from jax.experimental import pallas as pl
from jax.experimental.pallas import tpu as pltpu
from jax.sharding import Mesh, PartitionSpec as P


EXPERTS = 4
CAP = 20
MAIN = 16
TAIL = CAP - MAIN
QUARTERS = 4
CLASSES = 4
CORES = 2


def cost(flops, nbytes):
    return pl.CostEstimate(flops=flops, bytes_accessed=nbytes, transcendentals=0)


def count_at_least(index, width, parts):
    total = jnp.zeros_like(index)
    for k in range(1, parts):
        total = total + (index >= k * width).astype(jnp.int32)
    return total


def placed(ids, expert, slot, before):
    chosen = ((ids[0:1, :] == expert) | (ids[1:2, :] == expert)).astype(jnp.float32)
    position = jnp.dot(chosen, before, preferred_element_type=jnp.float32)
    return chosen * (position == slot.astype(jnp.float32)).astype(jnp.float32)


def grouped(row, groups):
    later = row >= groups * MAIN
    rest = row - groups * MAIN
    main = count_at_least(row, MAIN, groups)
    tail = count_at_least(rest, TAIL, groups)
    group = jnp.where(later, tail, main)
    slot = jnp.where(later, MAIN + rest - TAIL * tail, row - MAIN * main)
    return group, slot


def dispatch_kernel(chips, ids_ref, tokens_ref, out_ref):
    count = tokens_ref.shape[0]
    row = lax.broadcasted_iota(jnp.int32, (EXPERTS * CAP, count), 0)
    expert = count_at_least(row, CAP, EXPERTS)
    slot = row - CAP * expert
    first = lax.broadcasted_iota(jnp.int32, (count, count), 0)
    second = lax.broadcasted_iota(jnp.int32, (count, count), 1)
    before = (first < second).astype(jnp.float32)
    placement = placed(ids_ref[...], expert, slot, before).astype(jnp.bfloat16)
    slots = jnp.dot(placement, tokens_ref[...], preferred_element_type=jnp.float32).astype(
        jnp.bfloat16
    )
    per_expert = chips // EXPERTS
    for chip in range(chips):
        e = chip // per_expert
        out_ref[chip] = slots[e * CAP : (e + 1) * CAP]


def dispatch(ids, tokens, chips):
    count, features = tokens.shape
    return pl.pallas_call(
        functools.partial(dispatch_kernel, chips),
        out_shape=jax.ShapeDtypeStruct((chips, CAP, features), jnp.bfloat16),
        cost_estimate=cost(2 * EXPERTS * CAP * count * features, 200000),
        compiler_params=pltpu.CompilerParams(vmem_limit_bytes=60 << 20),
        name="dispatch",
    )(ids, tokens)


def gather_rows_kernel(in_ref, out_ref):
    chips = in_ref.shape[0]
    for chip in range(chips):
        out_ref[chip * MAIN : (chip + 1) * MAIN] = in_ref[chip, :MAIN]
        at = chips * MAIN + chip * TAIL
        out_ref[at : at + TAIL] = in_ref[chip, MAIN:]


def gather_rows(slots):
    chips, _, depth = slots.shape
    return pl.pallas_call(
        gather_rows_kernel,
        out_shape=jax.ShapeDtypeStruct((chips * CAP, depth), jnp.bfloat16),
        cost_estimate=cost(1000, 250000),
        compiler_params=pltpu.CompilerParams(vmem_limit_bytes=4 << 20),
        name="gather_rows",
    )(slots)


def mixing_kernel(chips, count, ids_ref, logits_ref, out_ref):
    lanes = ids_ref.shape[1]
    rows = chips * QUARTERS * CAP
    row = lax.broadcasted_iota(jnp.int32, (rows, lanes), 0)
    chip = count_at_least(row, QUARTERS * CAP, chips)
    quarter, slot = grouped(row - QUARTERS * CAP * chip, QUARTERS)
    expert = count_at_least(chip, chips // EXPERTS, EXPERTS)
    lane = lax.broadcasted_iota(jnp.int32, (rows, lanes), 1)
    own = (count_at_least(lane, count, QUARTERS) == quarter).astype(jnp.float32)
    first = lax.broadcasted_iota(jnp.int32, (lanes, lanes), 0)
    second = lax.broadcasted_iota(jnp.int32, (lanes, lanes), 1)
    same = count_at_least(first, count, QUARTERS) == count_at_least(second, count, QUARTERS)
    before = ((first < second) & same).astype(jnp.float32)
    ids = ids_ref[...]
    diff = logits_ref[0:1, :] - logits_ref[1:2, :]
    share = jnp.where(ids[0:1, :] == expert, jax.nn.sigmoid(diff), jax.nn.sigmoid(-diff))
    out_ref[...] = (placed(ids, expert, slot, before) * share * own).astype(jnp.bfloat16)


def mixing(ids, logits, chips):
    count = ids.shape[1]
    rows = chips * QUARTERS * CAP
    return pl.pallas_call(
        functools.partial(mixing_kernel, chips, count),
        out_shape=jax.ShapeDtypeStruct((rows, QUARTERS * count), jnp.bfloat16),
        cost_estimate=cost(2 * rows * 128 * 128, 200000),
        compiler_params=pltpu.CompilerParams(vmem_limit_bytes=8 << 20),
        name="mixing",
    )(jnp.tile(ids, (1, QUARTERS)), jnp.tile(logits, (1, QUARTERS)))


def class_at(distance):
    own = 2 * lax.axis_index("half") + lax.axis_index("odd")
    return lax.rem(own + CLASSES + distance, CLASSES)


def side_by_side(refs, b, parity):
    return jnp.concatenate(
        [ref[b, parity if ref.shape[1] > 1 else 0] for ref in refs], axis=1
    )


def multiply(total, tokens, refs, parity, start):
    for b in range(0, tokens.shape[0], 2):
        rows = jnp.concatenate([tokens[b], tokens[b + 1]], axis=1)
        weight = jnp.concatenate(
            [side_by_side(refs, start + b, parity), side_by_side(refs, start + b + 1, parity)],
            axis=0,
        )
        added = jnp.dot(rows, weight, preferred_element_type=jnp.float32)
        total = added if total is None else total + added
    return total


def own_kernel(slots_ref, gate_ref, gate2_ref, up_ref, up2_ref, out_ref, rest_ref):
    refs = (gate_ref, gate2_ref, up_ref, up2_ref)
    parity = lax.axis_index("odd")
    out_ref[...] = multiply(None, slots_ref, refs, parity, 0)
    for b in range(slots_ref.shape[0]):
        rest_ref[b, 0] = up2_ref[b, 1 - parity]


def own_part(slots, *weights):
    pairs, rows, depth = slots.shape
    width = weights[0].shape[-1]
    return pl.pallas_call(
        own_kernel,
        out_shape=(
            jax.ShapeDtypeStruct((rows, 4 * width), jnp.float32),
            jax.ShapeDtypeStruct((pairs, 1, depth, width), jnp.bfloat16),
        ),
        cost_estimate=cost(2 * pairs * rows * depth * 4 * width, 4200000),
        compiler_params=pltpu.CompilerParams(vmem_limit_bytes=16 << 20),
        name="own_part",
    )(slots, *weights)


def down_pair(hidden, refs, q, kind, depth):
    def block(q):
        lanes = pl.ds(pl.multiple_of((CLASSES * q + kind) * depth, 128), depth)
        return jnp.concatenate([ref[:, lanes] for ref in refs], axis=0)

    weight = jnp.concatenate([block(q), block(q + 1)], axis=1)
    return jnp.dot(hidden, weight, preferred_element_type=jnp.float32)


def ffn_kernel(
    total_ref, left_ref, right_ref, gate_ref, gate2_ref, up_ref, up2_ref, down_ref, down2_ref, hidden_ref, to_right_ref, to_left_ref, to_right2_ref, to_left2_ref
):
    pairs, _, depth = left_ref.shape
    parity = 1 - lax.axis_index("odd")
    width = gate_ref.shape[-1]
    half = QUARTERS // 2
    refs = (gate_ref, gate2_ref, up_ref, up2_ref)
    total = multiply(total_ref[...], left_ref, refs, parity, 0)
    total = multiply(total, right_ref, refs, parity, pairs)
    gate = total[:, : 2 * width]
    hidden = (gate * jax.nn.sigmoid(gate) * total[:, 2 * width :]).astype(jnp.bfloat16)
    hidden_ref[...] = hidden
    downs = (down_ref, down2_ref)
    for out_ref, distance, start in (
        (to_right_ref, 1, 0),
        (to_left_ref, -1, 0),
        (to_right2_ref, 2, 0),
        (to_left2_ref, 2, half),
    ):
        for b in range(0, out_ref.shape[0], 2):
            partial = down_pair(hidden, downs, start + b, class_at(distance), depth)
            partial = partial.astype(jnp.bfloat16)
            out_ref[b] = partial[:, :depth]
            out_ref[b + 1] = partial[:, depth:]


def ffn(total, left, right, *weights):
    rows, depth = left.shape[1:]
    width, model = weights[-1].shape
    sent = jax.ShapeDtypeStruct((QUARTERS, rows, depth), jnp.bfloat16)
    half = jax.ShapeDtypeStruct((QUARTERS // 2, rows, depth), jnp.bfloat16)
    return pl.pallas_call(
        ffn_kernel,
        out_shape=(
            jax.ShapeDtypeStruct((rows, 2 * width), jnp.bfloat16),
            sent,
            sent,
            half,
            half,
        ),
        cost_estimate=cost(2 * rows * model * width * 4, 9000000),
        compiler_params=pltpu.CompilerParams(vmem_limit_bytes=20 << 20),
        name="ffn",
    )(total, left, right, *weights)


def own_down_kernel(hidden_ref, down_ref, down2_ref, left_ref, right_ref, out_ref):
    blocks, _, depth = out_ref.shape
    for b in range(0, blocks, 2):
        partial = down_pair(hidden_ref[...], (down_ref, down2_ref), b, class_at(0), depth)
        for i, own in ((b, partial[:, :depth]), (b + 1, partial[:, depth:])):
            near = left_ref[i].astype(jnp.float32) + right_ref[i].astype(jnp.float32)
            out_ref[i] = own + near


def own_down(hidden, down, down2, left, right):
    rows = hidden.shape[0]
    width, model = down.shape
    depth = model // (CLASSES * QUARTERS)
    return pl.pallas_call(
        own_down_kernel,
        out_shape=jax.ShapeDtypeStruct((QUARTERS, rows, depth), jnp.float32),
        cost_estimate=cost(rows * model * width, 4000000),
        compiler_params=pltpu.CompilerParams(vmem_limit_bytes=16 << 20),
        name="own_down",
    )(hidden, down, down2, left, right)


def join_kernel(near_ref, left2_ref, right2_ref, out_ref):
    blocks = near_ref.shape[0]
    chips = out_ref.shape[0]
    half = blocks // 2
    for q in range(blocks):
        third = left2_ref[q] if q < half else right2_ref[q - half]
        both = (near_ref[q] + third.astype(jnp.float32)).astype(jnp.bfloat16)
        at = QUARTERS * MAIN + q * TAIL
        for chip in range(chips):
            tail = chips * MAIN + chip * TAIL
            out_ref[chip, q * MAIN : (q + 1) * MAIN] = both[chip * MAIN : (chip + 1) * MAIN]
            out_ref[chip, at : at + TAIL] = both[tail : tail + TAIL]


def join(near, left2, right2, chips):
    blocks, rows, depth = near.shape
    return pl.pallas_call(
        join_kernel,
        out_shape=jax.ShapeDtypeStruct((chips, blocks * CAP, depth), jnp.bfloat16),
        cost_estimate=cost(blocks * rows * depth, 12 * blocks * rows * depth),
        compiler_params=pltpu.CompilerParams(vmem_limit_bytes=16 << 20),
        name="join",
    )(near, left2, right2)


def combine_kernel(mix_ref, back_ref, out_ref):
    blocks, count, depth = out_ref.shape
    per_quarter = blocks // QUARTERS
    summed = lax.dot_general(
        mix_ref[...], back_ref[...], (((0,), (0,)), ((), ())), preferred_element_type=jnp.float32
    ).astype(jnp.bfloat16)
    for q in range(QUARTERS):
        for s in range(per_quarter):
            out_ref[q * per_quarter + s] = summed[
                q * count : (q + 1) * count, s * depth : (s + 1) * depth
            ]


def combine(mix, back, count, blocks):
    rows, quarter = back.shape
    depth = QUARTERS * quarter // blocks
    return pl.pallas_call(
        combine_kernel,
        out_shape=jax.ShapeDtypeStruct((blocks, count, depth), jnp.bfloat16),
        cost_estimate=cost(2 * rows * quarter * 128, 2400000),
        compiler_params=pltpu.CompilerParams(vmem_limit_bytes=12 << 20),
        name="combine",
    )(mix, back)


def on_device(tokens, expert_ids, route_logits, gate_weight, up_weight, down_weight):
    chips = lax.axis_size("x")
    pairs = lax.axis_size("quarter") * lax.axis_size("half")
    parts = 2 * pairs
    count, depth = tokens.shape
    swap = [(0, 1), (1, 0)]
    along = ("quarter", "half", "odd")
    ids = expert_ids.T

    def shift(value, distance):
        return lax.ppermute(value, along, [(i, (i + distance) % parts) for i in range(parts)])

    outgoing = dispatch(ids, tokens, chips)
    gate, up, down, outgoing = lax.optimization_barrier(
        (gate_weight, up_weight, down_weight, outgoing)
    )
    incoming = lax.all_to_all(outgoing, "x", 0, 0, tiled=True)
    gate2 = lax.ppermute(gate, "core", swap)
    up2 = lax.ppermute(up, "core", swap)
    down2 = lax.ppermute(down, "core", swap)
    own = lax.all_gather(gather_rows(incoming), ("quarter", "half"))
    left, right = shift(own[: pairs // 2], 1), shift(own[pairs // 2 :], -1)
    blocks = [w.reshape(pairs, 2, depth, w.shape[1]) for w in (gate, gate2, up, up2)]
    total, rest = own_part(own, *blocks)
    hidden, to_right, to_left, to_right2, to_left2 = ffn(
        total, left, right, *blocks[:3], rest, down, down2
    )
    left, right = shift(to_right, 1), shift(to_left, -1)
    left2, right2 = shift(to_right2, 2), shift(to_left2, -2)
    partial_value = join(own_down(hidden, down, down2, left, right), left2, right2, chips)
    returned = lax.all_to_all(partial_value, "x", 0, 0, tiled=True)
    mix = mixing(ids, route_logits.T, chips)
    combined = combine(mix, returned.reshape(chips * QUARTERS * CAP, depth), count, QUARTERS)
    blocks = lax.all_to_all(combined, "quarter", 0, 0, tiled=True)
    return jnp.sum(blocks.astype(jnp.float32), axis=0).astype(jnp.bfloat16)


def solution(mesh):
    sizes = [mesh.shape[axis] for axis in ("rep", "exp", "tp")]
    devices = mesh.devices.reshape(sizes[0], sizes[1] // CORES, CORES, QUARTERS, 2, 2)
    split = Mesh(devices, ("rep", "x", "core", "quarter", "half", "odd"))
    tokens = ("rep", "x", "core")
    features = ("quarter", "half", "odd")
    hidden = ("x", "core", "quarter", "half", "odd")
    return jax.shard_map(
        on_device,
        mesh=split,
        in_specs=(
            P(tokens, features),
            P(tokens, None),
            P(tokens, None),
            P(None, hidden),
            P(None, hidden),
            P(hidden, None),
        ),
        out_specs=P(tokens, features),
        check_vma=False,
    )
```
